32 devices in a mesh: mp: 8 (over z, x), dp: 4 (over y, core).
Axes of the slice: x: 2, y: 2, z: 4, core: 2. Of those that a mesh axis runs over, the one named last changes fastest.
Arguments:
- inputs: bfloat16 [6144, 512], P('mp', 'dp'), may hold values from -200 to 200
- norm_gain: float32 [6144], replicated, may hold values from 0.5 to 1.5
- norm_bias: float32 [6144], replicated, may hold values from -1.8 to 1.8
- proj_weight: bfloat16 [6144, 24576], P(None, 'mp'), may hold values from -0.078125 to 0.078125
- proj_bias: float32 [24576], P('mp'), may hold values from -3 to 3
- act_grad: bfloat16 [512, 24576], P('dp', 'mp'), may hold values from -6 to 6
Outputs:
- grad_inputs: bfloat16 [6144, 512], P('mp', 'dp')
- grad_weight: float32 [6144, 24576], P('dp', 'mp')
The draws below stay inside these ranges and needn't reach their ends.
All inputs are finite; a program needn't handle non-finite values.
Results may differ from the reference program's by a relative error of at most 0.017.
Values may be sent and summed in bfloat16 or wider, within the bound.
No kernel may reach another device: no remote copies, remote signals or barrier semaphores. Data moves between devices by JAX's collectives and lax.ppermute only.
A program may use at most 128 MiB of HBM per device.

```python
import math
import jax
import jax.numpy as jnp
from jax import lax

D = 6144
F = 24576
TOK_DEV = 128
TOKENS = 512
N_DP = 4


def draw_inputs(key, part):
    subkeys = jax.random.split(jax.random.fold_in(key, 17), 4)
    position = jnp.arange(D, dtype=jnp.float32) / D
    growth = math.log(3.0)
    jitter = jnp.clip(jax.random.normal(subkeys[0], (D, TOKENS), jnp.float32), -6.0, 6.0)
    channel = jnp.exp(growth * position + math.log(4.0) * jax.random.uniform(subkeys[1], (D,), jnp.float32))
    row_scale = jnp.exp(math.log(10.0) * jax.random.uniform(subkeys[2], (TOKENS,), jnp.float32))
    offset_rows = jnp.clip(jax.random.normal(subkeys[3], (TOKENS,), jnp.float32), -4.0, 4.0)
    values = row_scale[None, :] * (offset_rows[None, :] + channel[:, None] * jitter) * 0.25
    return values.astype(jnp.bfloat16)


def steps_of(own_key, shape, pieces, smallest, largest):
    factor_of, own = 1.0, jax.random.fold_in(own_key, 6)
    for dim, blocks in pieces:
        steps = jnp.exp(jax.random.uniform(jax.random.fold_in(own, dim), (blocks,), jnp.float32, smallest / len(pieces), largest / len(pieces)))
        factor_of = factor_of * jnp.repeat(steps, shape[dim] // blocks).reshape([-1 if axis == dim else 1 for axis in range(len(shape))])
    return factor_of


def gaussian(rng, extent, width, limit, pieces=(), kind=jnp.bfloat16):
    result = width * jax.random.normal(rng, extent, jnp.float32)
    if pieces:
        result = result * steps_of(rng, extent, pieces, -0.22, 0.18)
    return jnp.clip(result, -limit, limit).astype(kind)


def setup_inputs(seed: int = 0) -> dict:
    seeds = jax.random.split(jax.random.key(seed), 7)
    inputs = draw_inputs(jax.random.fold_in(seeds[6], 71), 0)
    norm_gain = jnp.clip(1.0 + 0.1 * jax.random.normal(seeds[1], (D,), jnp.float32), 0.5, 1.5)
    norm_bias = gaussian(seeds[2], (D,), 0.3, 1.8, (), jnp.float32)
    proj_weight = gaussian(seeds[3], (D, F), D ** -0.5, 0.078125, ((1, 8),))
    proj_bias = gaussian(seeds[4], (F,), 0.5, 3.0, ((0, 8),), jnp.float32)
    act_grad = gaussian(seeds[5], (TOKENS, F), 1.0, 6.0, ((0, 4), (1, 8)))
    return {"inputs": inputs, "norm_gain": norm_gain, "norm_bias": norm_bias, "proj_weight": proj_weight, "proj_bias": proj_bias, "act_grad": act_grad}


epsilon = 1e-06
root_half = 0.7071067811865476
density_norm = 0.3989422804014327

def gelu_slope(preact):
    cumulative = 0.5 * (1.0 + lax.erf(preact * root_half))
    return cumulative + preact * density_norm * jnp.exp(-0.5 * preact * preact)

def reference(inputs, norm_gain, norm_bias, proj_weight, proj_bias, act_grad):
    values = inputs.astype(jnp.float32)
    average = lax.optimization_barrier(jnp.sum(values, axis=0)) / D
    squares = lax.optimization_barrier(jnp.sum(values * values, axis=0)) / D
    inv_std = lax.rsqrt(squares - average * average + epsilon)
    centred = (values - average) * inv_std
    normed = (centred * norm_gain[:, None] + norm_bias[:, None]).astype(jnp.bfloat16)
    preact = lax.dot_general(normed, proj_weight, (((0,), (0,)), ((), ())), preferred_element_type=jnp.float32) + proj_bias
    pre_grad = (act_grad.astype(jnp.float32) * gelu_slope(preact)).astype(jnp.bfloat16)
    factor = 1.0 / math.sqrt(TOKENS)

    def add_block(block, running):
        offset = (block * TOK_DEV).astype(jnp.int32)
        rows_normed = lax.dynamic_slice_in_dim(normed, offset, TOK_DEV, 1)
        rows_grad = lax.dynamic_slice_in_dim(pre_grad, offset, TOK_DEV, 0)
        partial_sum = jnp.dot(rows_normed, rows_grad, preferred_element_type=jnp.float32) * factor
        rounded = lax.optimization_barrier(partial_sum.astype(jnp.bfloat16))
        return running + rounded.astype(jnp.float32)
    grad_weight = lax.fori_loop(0, N_DP, add_block, jnp.zeros((D, F), jnp.float32))
    input_grad = lax.dot_general(proj_weight, pre_grad, (((1,), (1,)), ((), ())), preferred_element_type=jnp.float32)
    scaled = input_grad * norm_gain[:, None]
    first_term = lax.optimization_barrier(jnp.sum(scaled, axis=0)) / D
    second_term = lax.optimization_barrier(jnp.sum(scaled * centred, axis=0)) / D
    grad_inputs = (inv_std * (scaled - first_term - centred * second_term)).astype(jnp.bfloat16)
    return (grad_inputs, grad_weight)
```

```python
import functools
import math

import jax
import jax.numpy as jnp
import numpy as np
from jax import lax
from jax.experimental import pallas as pl
from jax.experimental.pallas import tpu as pltpu
from jax.sharding import PartitionSpec as P


epsilon = 1e-06
root_half = 0.7071067811865476
density_norm = 0.3989422804014327
f32, bf16 = jnp.float32, jnp.bfloat16
VMEM_BYTES = 48 * 1024 * 1024


def params():
    return pltpu.CompilerParams(vmem_limit_bytes=VMEM_BYTES)


def cost(flops, moved):
    return pl.CostEstimate(flops=int(flops), bytes_accessed=int(moved), transcendentals=0)


def ring_of(size, columns):
    rows = size // columns
    if columns < 2 or rows < 2 or rows % 2 or size % columns:
        return list(range(size))
    walk = []
    for row in range(rows):
        inner = range(1, columns)
        walk += [row * columns + c for c in (inner if row % 2 == 0 else reversed(inner))]
    return walk + [row * columns for row in reversed(range(rows))]


def column_of(row):
    n = row.shape[1]
    step = 128 if n % 128 == 0 else n
    parts = [
        jnp.broadcast_to(row[:, i : i + step], (128, step)).T for i in range(0, n, step)
    ]
    return parts[0] if len(parts) == 1 else jnp.concatenate(parts, axis=0)


def gelu_slope(preact):
    cumulative = 0.5 * (1.0 + lax.erf(preact * root_half))
    return cumulative + preact * density_norm * jnp.exp(-0.5 * preact * preact)


def sums_kernel(x_ref, out_ref):
    values = x_ref[...].astype(f32)
    out_ref[0:1, :] = jnp.sum(values, axis=0, keepdims=True)
    out_ref[1:2, :] = jnp.sum(values * values, axis=0, keepdims=True)


def sums_of(x):
    return pl.pallas_call(
        sums_kernel,
        out_shape=jax.ShapeDtypeStruct((2, x.shape[1]), f32),
        compiler_params=params(),
        cost_estimate=cost(2 * x.size, 2 * x.size),
        name="sums",
    )(x)


def preact_kernel(count, n_sums, width, has_acc, last, *refs):
    refs = list(refs)
    table = refs.pop(0)
    xs = [refs.pop(0) for _ in range(count)]
    ws = [refs.pop(0) for _ in range(count)]
    gains = [refs.pop(0) for _ in range(count)]
    biases = [refs.pop(0) for _ in range(count)]
    sums = [refs.pop(0) for _ in range(n_sums)]
    stats_in = None if n_sums else refs.pop(0)
    acc_in = refs.pop(0) if has_acc else None
    if last:
        pbias, act = refs.pop(0), refs.pop(0)
    if has_acc:
        refs.pop(0)
    out = refs.pop(0)
    rows = refs.pop(0)
    stats_out = refs.pop(0) if n_sums else None
    turned = [refs.pop(0) for _ in range(count)]
    straight = [refs.pop(0) for _ in range(count)]
    sem = refs.pop(0)
    step = pl.program_id(0)

    @pl.when(step == 0)
    def _():
        if n_sums:
            total = sums[0][...]
            for s in sums[1:]:
                total = total + s[...]
            average = total[0:1, :] / width
            inv_std = lax.rsqrt(total[1:2, :] / width - average * average + epsilon)
            stats_out[0:1, :] = average
            stats_out[1:2, :] = inv_std
        else:
            average, inv_std = stats_in[0:1, :], stats_in[1:2, :]
        for e in range(count):
            centred = (xs[e][...].astype(f32) - average) * inv_std
            normed = centred * column_of(gains[e][0]) + column_of(biases[e][0])
            straight[e][...] = normed.astype(bf16)
            turned[e][...] = normed.T.astype(bf16)
        for e in range(count):
            pltpu.make_async_copy(straight[e], rows.at[table[e]], sem.at[e]).start()

    total = None
    for e in range(count):
        term = jnp.dot(turned[e][...], ws[e][...], preferred_element_type=f32)
        total = term if total is None else total + term
    if has_acc:
        total = total + acc_in[...]
    if last:
        preact = total + pbias[...]
        out[...] = (act[...].astype(f32) * gelu_slope(preact)).astype(bf16)
    else:
        out[...] = total

    @pl.when(step == pl.num_programs(0) - 1)
    def _():
        for e in range(count):
            pltpu.make_async_copy(straight[e], rows.at[table[e]], sem.at[e]).wait()


def preact_part(table, xs, weight, gain, bias, sums, stats, acc, rows, tile, span, last):
    count, (height, tokens) = len(xs), xs[0].shape
    blocks = gain.shape[0]
    first, tiles = span
    width = height * blocks
    whole = lambda shape: pl.BlockSpec(shape, lambda j, t: (0,) * len(shape))
    picked = lambda e: pl.BlockSpec((1, 1, height), lambda j, t: (t[e], 0, 0))
    args = list(xs)
    specs = [whole((height, tokens)) for _ in xs]
    for e in range(count):
        args.append(weight)
        specs.append(pl.BlockSpec((height, tile), lambda j, t, e=e: (t[e], j + first)))
    for vector in (gain, bias):
        for e in range(count):
            args.append(vector)
            specs.append(picked(e))
    if sums is not None:
        args += sums
        specs += [whole((2, tokens)) for _ in sums]
    else:
        args.append(stats)
        specs.append(whole((2, tokens)))
    aliases = {}
    if acc is not None:
        args.append(acc)
        specs.append(pl.BlockSpec((tokens, tile), lambda j, t: (0, j + first)))
    if last is not None:
        pbias, act = last
        args += [pbias, act]
        specs.append(pl.BlockSpec((1, tile), lambda j, t: (0, j + first)))
        specs.append(pl.BlockSpec((tokens, tile), lambda j, t: (0, j + first)))
    if acc is not None:
        aliases[1 + len(args)] = 1
        args.append(rows)
        specs.append(pl.BlockSpec(memory_space=pl.ANY))
    outs = [
        jax.ShapeDtypeStruct((tokens, tile * tiles), f32 if last is None else bf16),
        jax.ShapeDtypeStruct((blocks, height, tokens), bf16),
    ]
    out_specs = [
        pl.BlockSpec((tokens, tile), lambda j, t: (0, j)),
        pl.BlockSpec(memory_space=pl.ANY),
    ]
    if sums is not None:
        outs.append(jax.ShapeDtypeStruct((2, tokens), f32))
        out_specs.append(whole((2, tokens)))
    body = functools.partial(
        preact_kernel, count, len(sums) if sums is not None else 0, width,
        acc is not None, last is not None,
    )
    return pl.pallas_call(
        body,
        grid_spec=pltpu.PrefetchScalarGridSpec(
            num_scalar_prefetch=1,
            grid=(tiles,),
            in_specs=specs,
            out_specs=out_specs,
            scratch_shapes=[pltpu.VMEM((tokens, height), bf16)] * count
            + [pltpu.VMEM((height, tokens), bf16)] * count
            + [pltpu.SemaphoreType.DMA((count,))],
        ),
        out_shape=outs,
        input_output_aliases=aliases,
        compiler_params=params(),
        cost_estimate=cost(
            2 * count * height * tokens * tile * tiles,
            count * height * tile * tiles * 2 + tokens * tile * tiles * 8,
        ),
        name="preact",
    )(table, *args)


def back_kernel(count, pieces, *refs):
    refs = list(refs)
    refs.pop(0)
    xs = [refs.pop(0) for _ in range(count)]
    ws = [refs.pop(0) for _ in range(count)]
    gains = [refs.pop(0) for _ in range(count)]
    stats = refs.pop(0)
    pgs = [refs.pop(0) for _ in range(pieces)]
    outs = [refs.pop(0) for _ in range(count)]
    sums = refs.pop(0)
    step = pl.program_id(0)

    @pl.when(step == 0)
    def _():
        sums[...] = jnp.zeros_like(sums)

    average, inv_std = stats[0:1, :], stats[1:2, :]
    first, second = sums[0:1, :], sums[1:2, :]
    for e in range(count):
        total, at = None, 0
        for pg in pgs:
            wide = pg.shape[1]
            term = lax.dot_general(
                ws[e][:, at : at + wide], pg[...], (((1,), (1,)), ((), ())),
                preferred_element_type=f32,
            )
            total = term if total is None else total + term
            at += wide
        outs[e][...] = total
        scaled = total * column_of(gains[e][0])
        centred = (xs[e][...].astype(f32) - average) * inv_std
        first = first + jnp.sum(scaled, axis=0, keepdims=True)
        second = second + jnp.sum(scaled * centred, axis=0, keepdims=True)
    sums[0:1, :] = first
    sums[1:2, :] = second


def back_part(table, xs, weight, gain, stats, pgs):
    count, (height, tokens) = len(xs), xs[0].shape
    blocks, hidden = gain.shape[0], weight.shape[1]
    subs = 3 if height % (3 * 128) == 0 else 1
    sub = height // subs
    gain = gain.reshape(blocks * subs, 1, sub)
    whole = lambda shape: pl.BlockSpec(shape, lambda j, t: (0,) * len(shape))
    specs = [pl.BlockSpec((sub, tokens), lambda j, t: (j, 0)) for _ in xs]
    specs += [
        pl.BlockSpec((sub, hidden), lambda j, t, e=e: (t[e] * subs + j, 0)) for e in range(count)
    ]
    specs += [
        pl.BlockSpec((1, 1, sub), lambda j, t, e=e: (t[e] * subs + j, 0, 0)) for e in range(count)
    ]
    specs += [whole((2, tokens))] + [whole(pg.shape) for pg in pgs]
    return pl.pallas_call(
        functools.partial(back_kernel, count, len(pgs)),
        grid_spec=pltpu.PrefetchScalarGridSpec(
            num_scalar_prefetch=1,
            grid=(subs,),
            in_specs=specs,
            out_specs=[pl.BlockSpec((sub, tokens), lambda j, t: (j, 0)) for _ in xs]
            + [whole((2, tokens))],
        ),
        out_shape=[jax.ShapeDtypeStruct((height, tokens), f32) for _ in xs]
        + [jax.ShapeDtypeStruct((2, tokens), f32)],
        compiler_params=params(),
        cost_estimate=cost(
            4 * count * height * tokens * hidden, count * height * hidden * 2
        ),
        name="back",
    )(table, *xs, *([weight] * count), *([gain] * count), stats, *pgs)


def last_kernel(n_got, n_sums, width, *refs):
    refs = list(refs)
    refs.pop(0)
    x, gain, stats, own = (refs.pop(0) for _ in range(4))
    got = [refs.pop(0) for _ in range(n_got)]
    sums = [refs.pop(0) for _ in range(n_sums)]
    out = refs.pop(0)
    total = sums[0][...]
    for s in sums[1:]:
        total = total + s[...]
    first_term, second_term = total[0:1, :] / width, total[1:2, :] / width
    average, inv_std = stats[0:1, :], stats[1:2, :]
    grad = own[...]
    for g in got:
        grad = grad + g[...].astype(f32)
    scaled = grad * column_of(gain[0])
    centred = (x[...].astype(f32) - average) * inv_std
    out[...] = (inv_std * (scaled - first_term - centred * second_term)).astype(bf16)


def last_part(table, x, gain, stats, own, got, sums):
    height, tokens = x.shape
    whole = lambda a: pl.BlockSpec(a.shape, lambda j, t: (0,) * a.ndim)
    return pl.pallas_call(
        functools.partial(last_kernel, len(got), len(sums), height * gain.shape[0]),
        grid_spec=pltpu.PrefetchScalarGridSpec(
            num_scalar_prefetch=1,
            grid=(1,),
            in_specs=[whole(x), pl.BlockSpec((1, 1, height), lambda j, t: (t[0], 0, 0)), whole(stats), whole(own)]
            + [whole(g) for g in got]
            + [whole(s) for s in sums],
            out_specs=whole(x),
        ),
        out_shape=jax.ShapeDtypeStruct(x.shape, bf16),
        compiler_params=params(),
        cost_estimate=cost(10 * x.size, 12 * x.size),
        name="finish",
    )(table, x, gain, stats, own, *got, *sums)


def grad_kernel(count, factor, aliased, *refs):
    refs = list(refs)
    lefts = [refs.pop(0) for _ in range(count)]
    rights = [refs.pop(0) for _ in range(count)]
    if aliased:
        refs.pop(0)
    out, joined = refs
    tokens = rights[0].shape[0]

    @pl.when(pl.program_id(0) == 0)
    def _():
        for k in range(count):
            joined[k * tokens : (k + 1) * tokens, :] = rights[k][...]

    left = jnp.concatenate([l[...] for l in lefts], axis=1)
    out[...] = jnp.dot(left, joined[...], preferred_element_type=f32) * factor


def grad_part(lefts, rights, target, at, total_columns, factor):
    count = len(lefts)
    height, tokens = lefts[0].shape
    columns = rights[0].shape[1]
    tiles = 6 if height % (6 * 16) == 0 else 1
    tile = height // tiles
    specs = [pl.BlockSpec((tile, tokens), lambda i: (i, 0)) for _ in lefts]
    specs += [pl.BlockSpec((tokens, columns), lambda i: (0, 0)) for _ in rights]
    args = [*lefts, *rights]
    aliases = {}
    if target is not None:
        aliases = {len(args): 0}
        args.append(target)
        specs.append(pl.BlockSpec(memory_space=pl.ANY))
    return pl.pallas_call(
        functools.partial(grad_kernel, count, factor, target is not None),
        grid=(tiles,),
        in_specs=specs,
        out_specs=pl.BlockSpec((tile, columns), lambda i: (i, at)),
        out_shape=jax.ShapeDtypeStruct((height, total_columns), f32),
        scratch_shapes=[pltpu.VMEM((count * tokens, columns), bf16)],
        input_output_aliases=aliases,
        compiler_params=params(),
        cost_estimate=cost(
            2 * height * count * tokens * columns, height * columns * 4
        ),
        name="weight_grad",
    )(*args)


def on_device(inputs, norm_gain, norm_bias, proj_weight, proj_bias, act_grad):
    height, tokens = inputs.shape
    hidden = proj_weight.shape[1]
    n_mp, n_dp = lax.axis_size("mp"), lax.axis_size("dp")
    factor = 1.0 / math.sqrt(tokens * n_dp)
    ring = ring_of(n_mp, max(n_dp // 2, 1))
    place = {m: i for i, m in enumerate(ring)}
    ahead = [(ring[i], ring[(i + 1) % n_mp]) for i in range(n_mp)]
    behind = [(b, a) for a, b in ahead]
    far = n_mp // 2
    shifts = [0] + [s for d in range(1, far) for s in (-d, d)] + [-far]
    lookup = np.array([[ring[(place[m] + s) % n_mp] for s in shifts] for m in range(n_mp)], np.int32)
    table = lax.dynamic_index_in_dim(jnp.asarray(lookup), lax.axis_index("mp"), 0, keepdims=False)
    order = {s: i for i, s in enumerate(shifts)}
    pick = lambda which: jnp.stack([table[order[s]] for s in which]) if len(which) > 1 else lax.dynamic_slice_in_dim(table, order[which[0]], 1)

    def everyone(value):
        return [value] + [
            lax.ppermute(value, "mp", [(i, (i + k) % n_mp) for i in range(n_mp)])
            for k in range(1, n_mp)
        ]

    gain = norm_gain.reshape(n_mp, 1, height)
    bias = norm_bias.reshape(n_mp, 1, height)
    tile = hidden // 4 if hidden % 512 == 0 else hidden
    n_tiles = hidden // tile

    sums = everyone(sums_of(inputs))
    block = {0: inputs}
    for d in range(1, far + 1):
        block[-d] = lax.ppermute(block[-d + 1], "mp", ahead)
        if d < far:
            block[d] = lax.ppermute(block[d - 1], "mp", behind)

    groups = [[0]] + [[-d, d] for d in range(1, far)]
    acc = rows = stats = None
    for g, which in enumerate(groups):
        made = preact_part(
            pick(which), [block[s] for s in which], proj_weight, gain, bias,
            sums if g == 0 else None, stats, acc, rows, tile, (0, n_tiles), None,
        )
        if g == 0:
            acc, rows, stats = made
        else:
            acc, rows = made
    n_parts = 2 if n_tiles % 2 == 0 else 1
    pgs = []
    for part in range(n_parts):
        many = n_tiles // n_parts
        pg, rows = preact_part(
            pick([-far]), [block[-far]], proj_weight, gain, bias, None, stats, acc, rows, tile,
            (part * many, many), (proj_bias.reshape(1, hidden), act_grad),
        )
        pgs.append(pg)

    dp_me = lax.axis_index("dp")
    per = n_mp // n_dp
    swap = lambda value, k: lax.ppermute(value, "dp", [(i, i ^ k) for i in range(n_dp)])
    lefts = []
    for k in range(n_dp):
        mine = lax.dynamic_slice_in_dim(rows, (dp_me ^ k) * per, per, 0).reshape(per * height, tokens)
        lefts.append(swap(mine, k) if k else mine)
    rights = []
    for pg in pgs:
        pieces = {0: pg}
        for k in range(2, n_dp, 2):
            pieces[k] = swap(pg, k)
        for k in range(0, n_dp, 2):
            pieces[k + 1] = swap(pieces[k], 1)
        rights.append([pieces[k] for k in range(n_dp)])

    partial, own_sums = {}, []
    for d in range(far, -1, -1):
        which = [-far] if d == far else [d, -d] if d else [0]
        made = back_part(pick(which), [block[s] for s in which], proj_weight, gain, stats, pgs)
        for s, value in zip(which, made[:-1]):
            partial[s] = value
        own_sums.append(made[-1])
    half = height // 2
    own_total = own_sums[0]
    for s in own_sums[1:]:
        own_total = own_total + s
    back_sums = everyone(own_total)
    start = partial[-far].astype(bf16)
    up = lax.ppermute(start[:half], "mp", ahead)
    down = lax.ppermute(start[half:], "mp", behind)
    for d in range(far - 1, 0, -1):
        a, b = partial[d], partial[-d]
        if d == far - 1:
            a = jnp.concatenate([a[:half] + up.astype(f32), a[half:]], axis=0)
            b = jnp.concatenate([b[:half], b[half:] + down.astype(f32)], axis=0)
        else:
            a, b = a + up.astype(f32), b + down.astype(f32)
        up = lax.ppermute(a.astype(bf16), "mp", ahead)
        down = lax.ppermute(b.astype(bf16), "mp", behind)
    grad_inputs = last_part(pick([0]), inputs, gain, stats, partial[0], [up, down], back_sums)

    grad_weight = None
    for at, right in enumerate(rights):
        grad_weight = grad_part(lefts, right, grad_weight, at, hidden, factor)
    return (grad_inputs, grad_weight)


def solution(mesh):
    in_specs = (P("mp", "dp"), P(), P(), P(None, "mp"), P("mp"), P("dp", "mp"))
    out_specs = (P("mp", "dp"), P("dp", "mp"))
    return jax.shard_map(
        on_device, mesh=mesh, in_specs=in_specs, out_specs=out_specs, check_vma=False
    )
```

```python
import functools
import math

import jax
import jax.numpy as jnp
import numpy as np
from jax import lax
from jax.experimental import pallas as pl
from jax.experimental.pallas import tpu as pltpu
from jax.sharding import PartitionSpec as P


epsilon = 1e-06
root_half = 0.7071067811865476
density_norm = 0.3989422804014327
f32, bf16 = jnp.float32, jnp.bfloat16
VMEM_BYTES = 16 * 1024 * 1024
EXTRA = 16


def ring_of(size, columns):
    rows = size // columns
    if columns < 2 or rows < 2 or rows % 2 or size % columns:
        return list(range(size))
    walk = []
    for row in range(rows):
        inner = range(1, columns)
        walk += [row * columns + c for c in (inner if row % 2 == 0 else reversed(inner))]
    return walk + [row * columns for row in reversed(range(rows))]


def column_of(row):
    n = row.shape[1]
    step = 128 if n % 128 == 0 else n
    parts = [
        jnp.broadcast_to(row[:, i : i + step], (128, step)).T for i in range(0, n, step)
    ]
    return parts[0] if len(parts) == 1 else jnp.concatenate(parts, axis=0)


def row_of(column):
    return jnp.broadcast_to(column, (128, 128)).T[0:1, :]


def gelu_slope(preact):
    cumulative = 0.5 * (1.0 + lax.erf(preact * root_half))
    return cumulative + preact * density_norm * jnp.exp(-0.5 * preact * preact)


class Args:
    def __init__(self):
        self.values, self.specs = [], []

    def put(self, values, space=pltpu.VMEM):
        for value in values:
            self.values.append(value)
            self.specs.append(pl.BlockSpec(memory_space=space))
        return self


def run(body, args, outs, name, flops, moved, scratch=(), out_spaces=None, limit=VMEM_BYTES):
    spaces = out_spaces or [pltpu.VMEM] * len(outs)
    return pl.pallas_call(
        body,
        in_specs=args.specs,
        out_specs=[pl.BlockSpec(memory_space=s) for s in spaces],
        out_shape=outs,
        scratch_shapes=list(scratch),
        compiler_params=pltpu.CompilerParams(vmem_limit_bytes=limit),
        cost_estimate=pl.CostEstimate(
            flops=int(flops), bytes_accessed=int(moved), transcendentals=0
        ),
        name=name,
    )(*args.values)


shape_of = jax.ShapeDtypeStruct


def sums_of(x):
    def body(x_ref, out_ref):
        values = x_ref[...].astype(f32)
        out_ref[0:1, :] = jnp.sum(values, axis=0, keepdims=True)
        out_ref[1:2, :] = jnp.sum(values * values, axis=0, keepdims=True)

    args = Args().put([x])
    return run(body, args, [shape_of((2, x.shape[1]), f32)], "sums", 10**8, x.size * 2)[0]


def load_blocks(table, events, weight, height):
    count, hidden = len(events), weight.shape[1]

    def body(table_ref, w_ref, *refs):
        outs, sem = refs[:count], refs[count]
        copies = []
        for i, e in enumerate(events):
            at = pl.multiple_of(table_ref[0, e] * height, height)
            copies.append(
                pltpu.make_async_copy(w_ref.at[pl.ds(at, height), :], outs[i], sem.at[i])
            )
        for c in copies:
            c.start()
        for c in copies:
            c.wait()

    args = Args().put([table], pltpu.SMEM).put([weight], pl.ANY)
    outs = [pltpu.VMEM((height, hidden), bf16)] * count
    time_flops = 1.4e-6 * count * 4e14
    return run(
        body, args, outs, "load", time_flops, count * height * hidden * 2,
        [pltpu.SemaphoreType.DMA((count,))],
    )


def norm_blocks(table, events, xs, gain, bias, total, width):
    count, (height, tokens) = len(xs), xs[0].shape

    def body(table_ref, gain_ref, bias_ref, total_ref, *refs):
        x_refs = refs[:count]
        straight, turned = refs[count : 2 * count], refs[2 * count : 3 * count]
        stats = refs[3 * count]
        average = total_ref[0:1, :] / width
        inv_std = lax.rsqrt(total_ref[1:2, :] / width - average * average + epsilon)
        stats[0:1, :] = average
        stats[1:2, :] = inv_std
        for i, e in enumerate(events):
            at = table_ref[0, e]
            g, b = gain_ref[at], bias_ref[at]
            centred = (x_refs[i][...].astype(f32) - average) * inv_std
            normed = centred * column_of(g) + column_of(b)
            straight[i][...] = normed.astype(bf16)
            turned[i][0:tokens, :] = normed.T.astype(bf16)
            terms = []
            for v in (g, b):
                high = v.astype(bf16).astype(f32)
                terms += [high, v - high]
            terms.append(jnp.zeros((EXTRA - 4, height), f32))
            turned[i][tokens : tokens + EXTRA, :] = jnp.concatenate(terms, axis=0).astype(bf16)

    args = Args().put([table], pltpu.SMEM).put([gain, bias, total]).put(xs)
    outs = [shape_of((height, tokens), bf16)] * count
    outs += [shape_of((tokens + EXTRA, height), bf16)] * count
    outs += [shape_of((2, tokens), f32)]
    made = run(body, args, outs, "norm", 3e8 * count, 4 * count * height * tokens)
    return made[:count], made[count : 2 * count], made[2 * count]


def chunk_of(n, most):
    for parts in range(1, n + 1):
        if n % parts == 0 and n // parts <= most and (n // parts) % 128 == 0:
            return n // parts
    return n


def preact_add(turned, weights, acc):
    count, rows = len(turned), turned[0].shape[0]
    height, hidden = weights[0].shape
    step = chunk_of(hidden, 1024)

    def body(*refs):
        t_refs, w_refs = refs[:count], refs[count : 2 * count]
        acc_ref = refs[2 * count] if acc is not None else None
        out = refs[-1]

        def one(j, _):
            at = pl.ds(pl.multiple_of(j * step, step), step)
            total = acc_ref[:, at] if acc is not None else None
            for t, w in zip(t_refs, w_refs):
                term = jnp.dot(t[...], w[:, at], preferred_element_type=f32)
                total = term if total is None else total + term
            out[:, at] = total
            return 0

        lax.fori_loop(0, hidden // step, one, 0)

    args = Args().put(turned).put(weights)
    if acc is not None:
        args.put([acc])
    flops = 1.3e-6 * 4e14 * count
    return run(body, args, [shape_of((rows, hidden), f32)], "preact", flops, 10**6)[0]


def slope_part(turned, weight, acc, pbias, act, span):
    tokens = act.shape[0]
    first, wide = span
    step = chunk_of(wide, 512)

    def body(t_ref, w_ref, acc_ref, pbias_ref, act_ref, out, sums):
        def one(j, carry):
            one_sum, two_sum = carry
            here = pl.ds(pl.multiple_of(first + j * step, step), step)
            total = acc_ref[:, here] + jnp.dot(
                t_ref[...], w_ref[:, here], preferred_element_type=f32
            )
            inner = total[0:tokens, :]
            gain_sum = total[tokens : tokens + 1, :] + total[tokens + 1 : tokens + 2, :]
            bias_sum = total[tokens + 2 : tokens + 3, :] + total[tokens + 3 : tokens + 4, :]
            slope = gelu_slope(inner + pbias_ref[:, here])
            grad = (act_ref[:, here].astype(f32) * slope).astype(bf16)
            out[:, pl.ds(pl.multiple_of(j * step, step), step)] = grad
            wide_grad = grad.astype(f32)
            one_sum = one_sum + jnp.sum(wide_grad * gain_sum, axis=1, keepdims=True)
            two_sum = two_sum + jnp.sum(wide_grad * (inner - bias_sum), axis=1, keepdims=True)
            return one_sum, two_sum

        zero = jnp.zeros((tokens, 1), f32)
        one_sum, two_sum = lax.fori_loop(0, wide // step, one, (zero, zero))
        sums[0:1, :] = row_of(one_sum)
        sums[1:2, :] = row_of(two_sum)

    args = Args().put([turned, weight, acc, pbias, act])
    outs = [shape_of((tokens, wide), bf16), shape_of((2, tokens), f32)]
    return run(body, args, outs, "slope", 2e-6 * 4e14, 10**6)


def back_blocks(weights, pgs, kind):
    count, height, tokens = len(weights), weights[0].shape[0], pgs[0].shape[0]
    step = 256 if height % 256 == 0 else height

    def body(*refs):
        w_refs, pg_refs, outs = refs[:count], refs[count : count + len(pgs)], refs[count + len(pgs) :]

        def one(j, _):
            at = pl.ds(pl.multiple_of(j * step, step), step)
            for w, out in zip(w_refs, outs):
                total, column = None, 0
                for pg in pg_refs:
                    wide = pg.shape[1]
                    term = lax.dot_general(
                        w[at, column : column + wide], pg[...], (((1,), (1,)), ((), ())),
                        preferred_element_type=f32,
                    )
                    total = term if total is None else total + term
                    column += wide
                out[at, :] = total.astype(kind)
            return 0

        lax.fori_loop(0, height // step, one, 0)

    args = Args().put(weights).put(pgs)
    outs = [shape_of((height, tokens), kind)] * count
    return run(body, args, outs, "back", 1.3e-6 * 4e14 * count, 10**6)


def choose(table, columns, candidates, count_of=1):
    labels = [label for label, _ in candidates]
    arrays = [array for _, array in candidates]
    height, tokens = arrays[0].shape[-2:]

    def body(table_ref, *refs):
        inputs, outs = refs[: len(arrays)], refs[len(arrays) :]
        for i, column in enumerate(columns):
            wanted = table_ref[0, column]
            for label, ref in zip(labels, inputs):

                @pl.when(wanted == label)
                def _(ref=ref, i=i):
                    at = (i % (len(columns) // count_of)) * height
                    outs[i // (len(columns) // count_of)][at : at + height, :] = ref[...]

    args = Args().put([table], pltpu.SMEM).put(arrays)
    outs = [shape_of((len(columns) // count_of * height, tokens), bf16)] * count_of
    return run(body, args, outs, "choose", 2e8, 10**6)


def finish(table, x, gain, stats, own, got, total):
    height, tokens = x.shape
    width = height * gain.shape[0]

    def body(table_ref, x_ref, gain_ref, stats_ref, own_ref, total_ref, *refs):
        out = refs[-1]
        first_term, second_term = total_ref[0:1, :] / width, total_ref[1:2, :] / width
        average, inv_std = stats_ref[0:1, :], stats_ref[1:2, :]
        grad = own_ref[...]
        for g in refs[:-1]:
            grad = grad + g[...].astype(f32)
        scaled = grad * column_of(gain_ref[table_ref[0, 0]])
        centred = (x_ref[...].astype(f32) - average) * inv_std
        out[...] = (inv_std * (scaled - first_term - centred * second_term)).astype(bf16)

    args = Args().put([table], pltpu.SMEM).put([x, gain, stats, own, total]).put(got)
    return run(body, args, [shape_of(x.shape, bf16)], "finish", 5e8, 10**6)[0]


def grad_part(lefts, rights, target, at, total_columns, factor):
    count = len(lefts)
    height, tokens = lefts[0].shape
    columns = rights[0].shape[1]
    tiles = 6 if height % (6 * 16) == 0 else 1
    tile = height // tiles

    def body(*refs):
        refs = list(refs)
        left_refs, right_refs = refs[:count], refs[count : 2 * count]
        out, joined = refs[-2:]

        @pl.when(pl.program_id(0) == 0)
        def _():
            for k in range(count):
                joined[k * tokens : (k + 1) * tokens, :] = right_refs[k][...]

        left = jnp.concatenate([l[...] for l in left_refs], axis=1)
        out[...] = jnp.dot(left, joined[...], preferred_element_type=f32) * factor

    specs = [pl.BlockSpec((tile, tokens), lambda i: (i, 0)) for _ in lefts]
    specs += [pl.BlockSpec((tokens, columns), lambda i: (0, 0)) for _ in rights]
    args = [*lefts, *rights]
    aliases = {}
    if target is not None:
        aliases = {len(args): 0}
        args.append(target)
        specs.append(pl.BlockSpec(memory_space=pl.ANY))
    return pl.pallas_call(
        body,
        grid=(tiles,),
        in_specs=specs,
        out_specs=pl.BlockSpec((tile, columns), lambda i: (i, at)),
        out_shape=shape_of((height, total_columns), f32),
        scratch_shapes=[pltpu.VMEM((count * tokens, columns), bf16)],
        input_output_aliases=aliases,
        compiler_params=pltpu.CompilerParams(vmem_limit_bytes=VMEM_BYTES),
        cost_estimate=pl.CostEstimate(
            flops=int(5e-6 * 4e14), bytes_accessed=height * columns * 4, transcendentals=0
        ),
        name="weight_grad",
    )(*args)


class Plan:
    def __init__(self, n_mp, n_dp):
        ring = ring_of(n_mp, max(n_dp // 2, 1))
        place = {m: i for i, m in enumerate(ring)}
        self.ahead = [(ring[i], ring[(i + 1) % n_mp]) for i in range(n_mp)]
        self.behind = [(b, a) for a, b in self.ahead]
        self.far = far = n_mp // 2
        self.shifts = [0] + [s for d in range(1, far) for s in (-d, d)] + [-far]
        self.event = {s: i for i, s in enumerate(self.shifts)}
        self.per = per = n_mp // n_dp
        block_at = [[ring[(place[m] + s) % n_mp] for s in self.shifts] for m in range(n_mp)]
        event_of = [{b: e for e, b in enumerate(row)} for row in block_at]

        def slots(m, p):
            first = p // 2 * 2 * per
            return sorted(event_of[m][b] for b in range(first, first + 2 * per))

        self.evens = list(range(2, n_dp, 2))
        self.slot_step = [
            max(abs(self.shifts[slots(m, p)[j]]) for m in range(n_mp) for p in range(n_dp))
            for j in range(2 * per)
        ]
        rows = []
        self.column = {}
        for m in range(n_mp):
            for p in range(n_dp):
                row = list(block_at[m])
                for k in self.evens:
                    self.column["send", k] = len(row)
                    row += slots(m, p ^ k)
                mine = [p * per + i for i in range(per)] + [(p ^ 1) * per + i for i in range(per)]
                self.column["own"] = len(row)
                row += [event_of[m][b] for b in mine]
                self.column["sort"] = len(row)
                order = slots(m, p)
                row += [order.index(event_of[m][b]) for b in mine]
                rows.append(row)
        self.table = np.array(rows, np.int32).reshape(n_mp * n_dp, 1, -1)


def on_device(inputs, norm_gain, norm_bias, proj_weight, proj_bias, act_grad):
    height, tokens = inputs.shape
    hidden = proj_weight.shape[1]
    n_mp, n_dp = lax.axis_size("mp"), lax.axis_size("dp")
    width = height * n_mp
    factor = 1.0 / math.sqrt(tokens * n_dp)
    plan = Plan(n_mp, n_dp)
    far, per, shifts, event = plan.far, plan.per, plan.shifts, plan.event
    table = lax.dynamic_index_in_dim(
        jnp.asarray(plan.table), lax.axis_index("mp") * n_dp + lax.axis_index("dp"), 0, keepdims=False
    )
    gain = norm_gain.reshape(n_mp, 1, height)
    bias = norm_bias.reshape(n_mp, 1, height)
    swap = lambda value, k: lax.ppermute(value, "dp", [(i, i ^ k) for i in range(n_dp)])

    def summed(value):
        k = 1
        while k < n_mp:
            value = value + lax.ppermute(value, "mp", [(i, i ^ k) for i in range(n_mp)])
            k *= 2
        return value

    block = {0: inputs}
    for d in range(1, far + 1):
        block[-d] = lax.ppermute(block[-d + 1], "mp", plan.ahead)
        if d < far:
            block[d] = lax.ppermute(block[d - 1], "mp", plan.behind)
    total = summed(sums_of(inputs))

    early = min(2, far - 1)
    groups = [[e for e, s in enumerate(shifts) if abs(s) <= early]]
    groups += [[event[-d], event[d]] for d in range(early + 1, far)] + [[event[-far]]]
    weights, made, turned = {}, {}, {}
    half = max(len(shifts) // 2, 1)
    for some in (range(half), range(half, len(shifts))):
        for e, w in zip(some, load_blocks(table, list(some), proj_weight, height)):
            weights[e] = pltpu.with_memory_space_constraint(w, pltpu.VMEM)

    acc, stats, sent = None, None, {k: [] for k in plan.evens}
    slot = 0
    for events in groups:
        straight, sideways, stats = norm_blocks(
            table, events, [block[shifts[e]] for e in events], gain, bias, total, width
        )
        made.update(zip(events, straight))
        turned.update(zip(events, sideways))
        reach = max(abs(shifts[e]) for e in events)
        more = sum(1 for s in plan.slot_step[slot:] if s <= reach)
        if more:
            for k in plan.evens:
                first = plan.column["send", k] + slot
                picked = choose(table, list(range(first, first + more)), list(made.items()))[0]
                sent[k].append(swap(picked, k))
            slot += more
        if events is not groups[-1]:
            acc = preact_add([turned[e] for e in events], [weights[e] for e in events], acc)

    n_parts = 2 if hidden % 1024 == 0 else 1
    wide = hidden // n_parts
    last = len(shifts) - 1
    pgs, part_sums = [], []
    for part in range(n_parts):
        pg, s = slope_part(
            turned[last], weights[last], acc, proj_bias.reshape(1, hidden), act_grad, (part * wide, wide)
        )
        pgs.append(pg)
        part_sums.append(s)
    back_total = summed(functools.reduce(lambda a, b: a + b, part_sums))

    rights = []
    for pg in pgs:
        pieces = {0: pg}
        for k in plan.evens:
            pieces[k] = swap(pg, k)
        for k in [0, *plan.evens]:
            pieces[k + 1] = swap(pieces[k], 1)
        rights.append([pieces[k] for k in range(n_dp)])
    lefts = {}
    for k in [0, *plan.evens]:
        if k:
            arrived = jnp.concatenate(sent[k], axis=0).reshape(2 * per, height, tokens)
            candidates = [(j, arrived[j]) for j in range(2 * per)]
            first = plan.column["sort"]
        else:
            candidates = list(made.items())
            first = plan.column["own"]
        mine, other = choose(table, list(range(first, first + 2 * per)), candidates, 2)
        lefts[k] = mine
        lefts[k + 1] = swap(other, 1)
    lefts = [lefts[k] for k in range(n_dp)]

    up = lax.ppermute(back_blocks([weights[last]], pgs, bf16)[0], "mp", plan.ahead)
    down = None
    for d in range(far - 1, 0, -1):
        a, b = back_blocks([weights[event[d]], weights[event[-d]]], pgs, f32)
        a = a + up.astype(f32)
        b = b + down.astype(f32) if down is not None else b
        up = lax.ppermute(a.astype(bf16), "mp", plan.ahead)
        down = lax.ppermute(b.astype(bf16), "mp", plan.behind)
    own = back_blocks([weights[0]], pgs, f32)[0]
    got = [up] if down is None else [up, down]
    grad_inputs = finish(table, inputs, gain, stats, own, got, back_total)

    grad_weight = None
    for at, right in enumerate(rights):
        grad_weight = grad_part(lefts, right, grad_weight, at, hidden, factor)
    return (grad_inputs, grad_weight)


def solution(mesh):
    in_specs = (P("mp", "dp"), P(), P(), P(None, "mp"), P("mp"), P("dp", "mp"))
    out_specs = (P("mp", "dp"), P("dp", "mp"))
    return jax.shard_map(
        on_device, mesh=mesh, in_specs=in_specs, out_specs=out_specs, check_vma=False
    )
```

```python
import math

import jax
import jax.numpy as jnp
import numpy as np
from jax import lax
from jax.experimental import pallas as pl
from jax.experimental.pallas import tpu as pltpu
from jax.sharding import PartitionSpec as P


epsilon = 1e-06
root_half = 0.7071067811865476
density_norm = 0.3989422804014327
f32, bf16 = jnp.float32, jnp.bfloat16
VMEM_BYTES = 8 * 1024 * 1024
PIECES = 1
EXTRA = 16


def ring_of(size, columns):
    rows = size // columns
    if columns < 2 or rows < 2 or rows % 2 or size % columns:
        return list(range(size))
    walk = []
    for row in range(rows):
        inner = range(1, columns)
        walk += [row * columns + c for c in (inner if row % 2 == 0 else reversed(inner))]
    return walk + [row * columns for row in reversed(range(rows))]


def column_of(row):
    n = row.shape[1]
    step = 128 if n % 128 == 0 else n
    parts = [
        jnp.broadcast_to(row[:, i : i + step], (128, step)).T for i in range(0, n, step)
    ]
    return parts[0] if len(parts) == 1 else jnp.concatenate(parts, axis=0)


def row_of(column):
    return jnp.broadcast_to(column, (128, 128)).T[0:1, :]


def gelu_slope(preact):
    cumulative = 0.5 * (1.0 + lax.erf(preact * root_half))
    return cumulative + preact * density_norm * jnp.exp(-0.5 * preact * preact)


class Args:
    def __init__(self):
        self.values, self.specs = [], []

    def put(self, values, space=pltpu.VMEM):
        for value in values:
            self.values.append(value)
            self.specs.append(pl.BlockSpec(memory_space=space))
        return self


def run(body, args, outs, flops, moved, scratch=(), out_spaces=None, limit=VMEM_BYTES):
    spaces = out_spaces or [pltpu.VMEM] * len(outs)
    return pl.pallas_call(
        body,
        in_specs=args.specs,
        out_specs=[pl.BlockSpec(memory_space=s) for s in spaces],
        out_shape=outs,
        scratch_shapes=list(scratch),
        compiler_params=pltpu.CompilerParams(vmem_limit_bytes=limit),
        cost_estimate=pl.CostEstimate(
            flops=int(flops), bytes_accessed=int(moved), transcendentals=0
        ),
    )(*args.values)


shape_of = jax.ShapeDtypeStruct


def sums_of(xs):
    count, tokens = len(xs), xs[0].shape[1]

    def body(*refs):
        out = refs[-1]
        one = two = None
        for i, x_ref in enumerate(refs[:-1]):
            values = x_ref[...].astype(f32)
            a = jnp.sum(values, axis=0, keepdims=True)
            b = jnp.sum(values * values, axis=0, keepdims=True)
            out[2 * i : 2 * i + 1, :] = a
            out[2 * i + 1 : 2 * i + 2, :] = b
            one, two = (a, b) if one is None else (one + a, two + b)
        out[2 * count : 2 * count + 1, :] = one
        out[2 * count + 1 : 2 * count + 2, :] = two

    outs = [shape_of((2 * count + 2, tokens), f32)]
    return run(body, Args().put(xs), outs, 4e8, 10**6)[0]


def total_of(parts):
    one = two = None
    for ref, row in parts:
        a, b = ref[row : row + 1, :], ref[row + 1 : row + 2, :]
        one, two = (a, b) if one is None else (one + a, two + b)
    return one, two


def split(one, two):
    terms = []
    for v in (one, two):
        high = v.astype(bf16).astype(f32)
        terms += [high, v - high]
    terms.append(jnp.zeros((EXTRA - 4, one.shape[1]), f32))
    return jnp.concatenate(terms, axis=0).astype(bf16)


def merge(ref, height):
    rows = ref[height : height + EXTRA, :].astype(f32)
    return rows[0:1, :] + rows[1:2, :], rows[2:3, :] + rows[3:4, :]


class Loads:
    def __init__(self, table, events, weight, height):
        self.table, self.events, self.weight, self.height = table, events, weight, height
        self.outs = [pltpu.VMEM((height, weight.shape[1]), bf16)] * len(events)

    def copies(self, table_ref, w_ref, outs, sem):
        made, piece = [], self.height // PIECES
        for i, e in enumerate(self.events):
            for j in range(PIECES):
                at = pl.multiple_of(table_ref[0, e] * self.height + j * piece, piece)
                made.append(
                    pltpu.make_async_copy(
                        w_ref.at[pl.ds(at, piece), :], outs[i].at[j * piece : (j + 1) * piece, :],
                        sem.at[i * PIECES + j],
                    )
                )
        return made

    @property
    def scratch(self):
        return [pltpu.SemaphoreType.DMA((max(len(self.events), 1) * PIECES,))]


def load_blocks(loads):
    def body(table_ref, w_ref, *refs):
        copies = loads.copies(table_ref, w_ref, refs[:-1], refs[-1])
        for c in copies:
            c.start()
        for c in copies:
            c.wait()

    args = Args().put([loads.table], pltpu.SMEM).put([loads.weight], pltpu.HBM)
    return run(body, args, loads.outs, 1e8, 10**6, loads.scratch, limit=8 * 1024 * 1024)


def normalize(x_ref, g, b, average, inv_std, straight, turned):
    tokens = x_ref.shape[1]
    centred = (x_ref[...].T.astype(f32) - average) * inv_std
    normed = (centred * g + b).astype(bf16)
    turned[0:tokens, :] = normed
    turned[tokens : tokens + EXTRA, :] = split(g, b)
    straight[...] = normed.T


def chunk_of(n, most):
    for parts in range(1, n + 1):
        if n % parts == 0 and n // parts <= most and (n // parts) % 128 == 0:
            return n // parts
    return n


def stats_of(refs, rows, width):
    one, two = total_of(list(zip(refs, rows)))
    average = one / width
    return average, lax.rsqrt(two / width - average * average + epsilon)


def stats_columns(average, inv_std):
    return tuple(jnp.broadcast_to(v, (128, v.shape[1])).T[:, 0:1] for v in (average, inv_std))


def pick(table_ref, columns, labels, refs, out, height):
    for i, column in enumerate(columns):
        wanted = table_ref[0, column]
        for label, ref in zip(labels, refs):

            @pl.when(wanted == label)
            def _(ref=ref, i=i):
                out[i * height : (i + 1) * height, :] = ref[...]


def norm_blocks(table, events, xs, gain, bias, sums, pool, picks):
    count, (height, tokens) = len(xs), xs[0].shape
    width = height * gain.shape[0]
    sum_arrays, sum_rows = [v for v, _ in sums], [r for _, r in sums]
    labels = [e for e, _ in pool] + list(events)

    def body(table_ref, gain_ref, bias_ref, *refs):
        refs = list(refs)
        take = lambda n: [refs.pop(0) for _ in range(n)]
        x_refs, sum_refs, pool_refs = take(count), take(len(sums)), take(len(pool))
        straight, turned, picked = take(count), take(count), refs
        columns = stats_columns(*stats_of(sum_refs, sum_rows, width))
        for i, e in enumerate(events):
            g, b = gain_ref[table_ref[0, e]], bias_ref[table_ref[0, e]]
            normalize(x_refs[i], g, b, *columns, straight[i], turned[i])
        for wanted, target in zip(picks, picked):
            pick(table_ref, wanted, labels, pool_refs + straight, target, height)

    args = Args().put([table], pltpu.SMEM).put([gain, bias]).put(xs).put(sum_arrays)
    args.put([array for _, array in pool])
    outs = [shape_of((height, tokens), bf16)] * count
    outs += [shape_of((tokens + EXTRA, height), bf16)] * count
    outs += [shape_of((len(wanted) * height, tokens), bf16) for wanted in picks]
    made = run(body, args, outs, 1e8 * count, 10**6)
    return made[:count], made[count : 2 * count], made[2 * count :]


def preact_add(turned, weights, acc, loads):
    count, ready = len(turned), len(weights)
    late = count - ready
    rows = turned[0].shape[0]
    hidden = loads.weight.shape[1]
    step = chunk_of(hidden, 1536 if count > 2 else 1024)
    n_loads = len(loads.events)

    def body(table_ref, w_any, *refs):
        refs = list(refs)
        take = lambda n: [refs.pop(0) for _ in range(n)]
        t_refs, w_refs = take(count), take(ready)
        acc_ref = take(1)[0] if acc is not None else None
        out, loaded, sem = take(1)[0], take(n_loads), refs[0]
        copies = loads.copies(table_ref, w_any, loaded, sem)
        for c in copies:
            c.start()

        def add(pairs, base):
            def one(j, _):
                at = pl.ds(pl.multiple_of(j * step, step), step)
                total = base[:, at] if base is not None else None
                for t, w in pairs:
                    term = jnp.dot(t[...], w[:, at], preferred_element_type=f32)
                    total = term if total is None else total + term
                out[:, at] = total
                return 0

            lax.fori_loop(0, hidden // step, one, 0, unroll=len(pairs) <= 2)

        if ready:
            add(list(zip(t_refs, w_refs)), acc_ref)
        for c in copies[: late * PIECES]:
            c.wait()
        if late:
            add(list(zip(t_refs[ready:], loaded)), out if ready else acc_ref)
        for c in copies[late * PIECES :]:
            c.wait()

    args = Args().put([loads.table], pltpu.SMEM).put([loads.weight], pltpu.HBM).put(turned).put(weights)
    if acc is not None:
        args.put([acc])
    outs = [shape_of((rows, hidden), f32)] + loads.outs
    made = run(body, args, outs, 2e8 * count, 10**6, loads.scratch)
    return made[0], made[1:]


def slopes(table, event, x, weight, gain, bias, sums, acc, pbias, act, n_parts, pool, picks):
    height, tokens = x.shape
    hidden = weight.shape[1]
    width = height * gain.shape[0]
    wide = hidden // n_parts
    step = chunk_of(wide, 512)
    labels = [e for e, _ in pool] + [event]
    sum_arrays, sum_rows = [v for v, _ in sums], [r for _, r in sums]

    def body(table_ref, gain_ref, bias_ref, x_ref, w_ref, acc_ref, pbias_ref, act_ref, *refs):
        refs = list(refs)
        take = lambda n: [refs.pop(0) for _ in range(n)]
        sum_refs, pool_refs, outs = take(len(sums)), take(len(pool)), take(n_parts)
        sums_out, stats, straight = take(3)
        picked, turned = take(len(picks)), refs[0]
        average, inv_std = stats_of(sum_refs, sum_rows, width)
        stats[0:1, :] = average
        stats[1:2, :] = inv_std
        g, b = gain_ref[table_ref[0, event]], bias_ref[table_ref[0, event]]
        normalize(x_ref, g, b, *stats_columns(average, inv_std), straight, turned)
        for wanted, target in zip(picks, picked):
            pick(table_ref, wanted, labels, pool_refs + [straight], target, height)
        one_sum = two_sum = jnp.zeros((tokens, 1), f32)
        for part, out in enumerate(outs):

            def one(j, carry, part=part, out=out):
                one_sum, two_sum = carry
                here = pl.ds(pl.multiple_of(part * wide + j * step, step), step)
                total = acc_ref[:, here] + jnp.dot(
                    turned[...], w_ref[:, here], preferred_element_type=f32
                )
                inner = total[0:tokens, :]
                gain_sum = total[tokens : tokens + 1, :] + total[tokens + 1 : tokens + 2, :]
                bias_sum = total[tokens + 2 : tokens + 3, :] + total[tokens + 3 : tokens + 4, :]
                slope = gelu_slope(inner + pbias_ref[:, here])
                grad = (act_ref[:, here].astype(f32) * slope).astype(bf16)
                out[:, pl.ds(pl.multiple_of(j * step, step), step)] = grad
                wide_grad = grad.astype(f32)
                one_sum = one_sum + jnp.sum(wide_grad * gain_sum, axis=1, keepdims=True)
                two_sum = two_sum + jnp.sum(wide_grad * (inner - bias_sum), axis=1, keepdims=True)
                return one_sum, two_sum

            one_sum, two_sum = lax.fori_loop(0, wide // step, one, (one_sum, two_sum), unroll=True)
        sums_out[0:1, :] = row_of(one_sum)
        sums_out[1:2, :] = row_of(two_sum)

    args = Args().put([table], pltpu.SMEM).put([gain, bias, x, weight, acc, pbias, act]).put(sum_arrays)
    args.put([array for _, array in pool])
    outs = [shape_of((tokens, wide), bf16)] * n_parts + [shape_of((2, tokens), f32)] * 2
    outs += [shape_of((height, tokens), bf16)]
    outs += [shape_of((len(wanted) * height, tokens), bf16) for wanted in picks]
    made = run(body, args, outs, 8e8, 10**6, [pltpu.VMEM((tokens + EXTRA, height), bf16)])
    return made[:n_parts], made[n_parts], made[n_parts + 1], made[n_parts + 2], made[n_parts + 3 :]


def back_blocks(weights, pgs, sums, as_message):
    count, height, tokens = len(weights), weights[0].shape[0], pgs[0].shape[0]
    step = 256 if height % 256 == 0 else height

    def body(sums_ref, *refs):
        w_refs, pg_refs, outs = refs[:count], refs[count : count + len(pgs)], refs[count + len(pgs) :]

        def one(j, _):
            at = pl.ds(pl.multiple_of(j * step, step), step)
            for w, out in zip(w_refs, outs):
                total, column = None, 0
                for pg in pg_refs:
                    wide = pg.shape[1]
                    term = lax.dot_general(
                        w[at, column : column + wide], pg[...], (((1,), (1,)), ((), ())),
                        preferred_element_type=f32,
                    )
                    total = term if total is None else total + term
                    column += wide
                out[at, :] = total.astype(out.dtype)
            return 0

        lax.fori_loop(0, height // step, one, 0, unroll=True)
        for i in range(count):
            if as_message[i]:
                outs[i][height : height + EXTRA, :] = split(sums_ref[0:1, :], sums_ref[1:2, :])

    args = Args().put([sums]).put(weights).put(pgs)
    outs = [
        shape_of((height + EXTRA, tokens), bf16) if m else shape_of((height, tokens), f32)
        for m in as_message
    ]
    return run(body, args, outs, 2e8 * count, 10**6)


def add_message(part, got, sums):
    height, _ = part.shape

    def body(part_ref, got_ref, sums_ref, out):
        out[0:height, :] = (part_ref[...] + got_ref[0:height, :].astype(f32)).astype(bf16)
        one, two = merge(got_ref, height)
        out[height : height + EXTRA, :] = split(one + sums_ref[0:1, :], two + sums_ref[1:2, :])

    args = Args().put([part, got, sums])
    return run(body, args, [shape_of(got.shape, bf16)], 1e8, 10**6)[0]


def choose(table, columns, candidates, count_of=1):
    labels = [label for label, _ in candidates]
    arrays = [array for _, array in candidates]
    height, tokens = arrays[0].shape[-2:]

    def body(table_ref, *refs):
        inputs, outs = refs[: len(arrays)], refs[len(arrays) :]
        for i, column in enumerate(columns):
            wanted = table_ref[0, column]
            for label, ref in zip(labels, inputs):

                @pl.when(wanted == label)
                def _(ref=ref, i=i):
                    at = (i % (len(columns) // count_of)) * height
                    outs[i // (len(columns) // count_of)][at : at + height, :] = ref[...]

    args = Args().put([table], pltpu.SMEM).put(arrays)
    outs = [shape_of((len(columns) // count_of * height, tokens), bf16)] * count_of
    return run(body, args, outs, 2e8, 10**6)


def back_own(table, weight, pgs, x, gain, stats):
    height, tokens = x.shape

    def body(table_ref, w_ref, x_ref, gain_ref, stats_ref, *refs):
        pg_refs, (own, columns, centred) = refs[: len(pgs)], refs[len(pgs) :]
        total, at = None, 0
        for pg in pg_refs:
            term = lax.dot_general(
                w_ref[:, at : at + pg.shape[1]], pg[...], (((1,), (1,)), ((), ())),
                preferred_element_type=f32,
            )
            total = term if total is None else total + term
            at += pg.shape[1]
        own[...] = total
        columns[...] = column_of(gain_ref[table_ref[0, 0]])
        centred[...] = (x_ref[...].astype(f32) - stats_ref[0:1, :]) * stats_ref[1:2, :]

    args = Args().put([table], pltpu.SMEM).put([weight, x, gain, stats]).put(pgs)
    return run(body, args, [shape_of((height, tokens), f32)] * 3, 3e8, 10**6)


def finish(own, columns, centred, stats, got, sums, width):
    height = own.shape[0]

    def body(own_ref, columns_ref, centred_ref, stats_ref, sums_ref, *refs):
        out = refs[-1]
        one, two = sums_ref[0:1, :], sums_ref[1:2, :]
        grad = own_ref[...]
        for g in refs[:-1]:
            grad = grad + g[0:height, :].astype(f32)
            a, b = merge(g, height)
            one, two = one + a, two + b
        first_term, second_term = one / width, two / width
        scaled = grad * columns_ref[...]
        out[...] = (
            stats_ref[1:2, :] * (scaled - first_term - centred_ref[...] * second_term)
        ).astype(bf16)

    args = Args().put([own, columns, centred, stats, sums]).put(got)
    return run(body, args, [shape_of(own.shape, bf16)], 3e8, 10**6)[0]


def grad_part(lefts, rights, target, span, tile, factor):
    count = len(lefts)
    height, tokens = lefts[0].shape
    columns = rights[0].shape[1]
    n_tiles = span[1] - span[0]
    slots = min(4, n_tiles)

    def body(*refs):
        refs = list(refs)
        left_refs, right_refs = refs[:count], refs[count : 2 * count]
        out, joined, made, sem = refs[-4:]
        for k in range(count):
            joined[k * tokens : (k + 1) * tokens, :] = right_refs[k][...]
        copies = []
        for i in range(n_tiles):
            at = slice((span[0] + i) * tile, (span[0] + i + 1) * tile)
            slot = i % slots
            if i >= slots:
                copies[i - slots].wait()
            left = jnp.concatenate([l[at, :] for l in left_refs], axis=1)
            made[slot] = jnp.dot(left, joined[...], preferred_element_type=f32) * factor
            copies.append(pltpu.make_async_copy(made.at[slot], out.at[at, :], sem.at[slot]))
            copies[-1].start()
        for c in copies[max(n_tiles - slots, 0) :]:
            c.wait()

    specs = [pl.BlockSpec(memory_space=pltpu.VMEM) for _ in lefts + rights]
    args = [*lefts, *rights]
    aliases = {}
    if target is not None:
        aliases = {len(args): 0}
        args.append(target)
        specs.append(pl.BlockSpec(memory_space=pltpu.HBM))
    return pl.pallas_call(
        body,
        in_specs=specs,
        out_specs=pl.BlockSpec(memory_space=pltpu.HBM),
        out_shape=shape_of((height, columns), f32),
        scratch_shapes=[
            pltpu.VMEM((count * tokens, columns), bf16),
            pltpu.VMEM((slots, tile, columns), f32),
            pltpu.SemaphoreType.DMA((slots,)),
        ],
        input_output_aliases=aliases,
        compiler_params=pltpu.CompilerParams(vmem_limit_bytes=28 * 1024 * 1024),
        cost_estimate=pl.CostEstimate(flops=int(5e8), bytes_accessed=10**6, transcendentals=0),
        name="weight_grad",
    )(*args)


class Plan:
    def __init__(self, n_mp, n_dp):
        ring = ring_of(n_mp, max(n_dp // 2, 1))
        place = {m: i for i, m in enumerate(ring)}
        self.ring = ring
        self.far = far = n_mp // 2
        self.shifts = [0] + [s for d in range(1, far) for s in (-d, d)] + [-far]
        self.event = {s: i for i, s in enumerate(self.shifts)}
        self.per = per = n_mp // n_dp
        block_at = [[ring[(place[m] + s) % n_mp] for s in self.shifts] for m in range(n_mp)]
        event_of = [{b: e for e, b in enumerate(row)} for row in block_at]

        def slots(m, p):
            first = p // 2 * 2 * per
            return sorted(event_of[m][b] for b in range(first, first + 2 * per))

        self.evens = list(range(2, n_dp, 2))
        self.slot_step = [
            max(abs(self.shifts[slots(m, p)[j]]) for m in range(n_mp) for p in range(n_dp))
            for j in range(2 * per)
        ]
        rows = []
        self.column = {}
        for m in range(n_mp):
            for p in range(n_dp):
                row = list(block_at[m])
                for k in self.evens:
                    self.column["send", k] = len(row)
                    row += slots(m, p ^ k)
                mine = [p * per + i for i in range(per)] + [(p ^ 1) * per + i for i in range(per)]
                self.column["own"] = len(row)
                row += [event_of[m][b] for b in mine]
                self.column["sort"] = len(row)
                order = slots(m, p)
                row += [order.index(event_of[m][b]) for b in mine]
                rows.append(row)
        self.table = np.array(rows, np.int32).reshape(n_mp * n_dp, 1, -1)


def on_device(inputs, norm_gain, norm_bias, proj_weight, proj_bias, act_grad):
    height, tokens = inputs.shape
    hidden = proj_weight.shape[1]
    n_mp, n_dp = lax.axis_size("mp"), lax.axis_size("dp")
    width = height * n_mp
    factor = 1.0 / math.sqrt(tokens * n_dp)
    plan = Plan(n_mp, n_dp)
    far, per, shifts, event = plan.far, plan.per, plan.shifts, plan.event
    table = lax.dynamic_index_in_dim(
        jnp.asarray(plan.table), lax.axis_index("mp") * n_dp + lax.axis_index("dp"), 0, keepdims=False
    )
    gain = norm_gain.reshape(n_mp, 1, height)
    bias = norm_bias.reshape(n_mp, 1, height)
    pbias = proj_bias.reshape(1, hidden)
    proj_weight = pltpu.with_memory_space_constraint(proj_weight, pltpu.HBM)

    def swap(value, k):
        return lax.ppermute(value, "dp", [(i, i ^ k) for i in range(n_dp)])

    def along(value, steps):
        pairs = [(plan.ring[i], plan.ring[(i + steps) % n_mp]) for i in range(n_mp)]
        return lax.ppermute(value, "mp", pairs)

    block = {0: inputs}
    for d in range(1, far + 1):
        block[-d] = along(block[-d + 1], 1)
        if d < far:
            block[d] = along(block[d - 1], -1)

    groups = [[0]] + [[event[-d], event[d]] for d in range(1, far)] + [[event[-far]]]
    early = min(2, far - 1)
    groups[: early + 1] = [sum(groups[: early + 1], [])]
    if far == 4:
        window = sums_of([block[0], block[-1], block[1]])
        below = along(window, 3)
        above = along(window, -3)
        sums = [(window, 6), (below, 6), (above, 0), (above, 2)]
    else:
        total, k = sums_of([inputs])[0:2], 1
        while k < n_mp:
            total = total + lax.ppermute(total, "mp", [(i, i ^ k) for i in range(n_mp)])
            k *= 2
        sums = [(total, 0)]

    weights, made = {}, {}

    def keep(events, arrays):
        for e, w in zip(events, arrays):
            weights[e] = pltpu.with_memory_space_constraint(w, pltpu.VMEM)

    first_loads = groups[0][:3]
    keep(first_loads, load_blocks(Loads(table, first_loads, proj_weight, height)))
    more_loads = groups[0][3 : 3 + 2]
    if more_loads:
        keep(more_loads, load_blocks(Loads(table, more_loads, proj_weight, height)))
    acc, sent, slot = None, {k: [] for k in plan.evens}, 0

    def ready_picks(reach):
        nonlocal slot
        more = sum(1 for s in plan.slot_step[slot:] if s <= reach)
        firsts = [plan.column["send", k] + slot for k in plan.evens] if more else []
        slot += more
        return [list(range(first, first + more)) for first in firsts]

    def send(picked):
        for k, value in zip(plan.evens, picked):
            sent[k].append(swap(value, k))

    waiting = []
    for g, events in enumerate(groups[:-1]):
        reach = max(abs(shifts[e]) for e in events)
        picks = ready_picks(reach)
        straight, turned, picked = norm_blocks(
            table, events, [block[shifts[e]] for e in events], gain, bias, sums,
            list(made.items()) if picks else [], picks,
        )
        made.update(zip(events, straight))
        send(picked)
        waiting += zip(events, turned)
        if len(groups) == 3 and g == 0:
            continue
        waiting.sort(key=lambda pair: pair[0] not in weights)
        late = [e for e, _ in waiting if e not in weights]
        loads = Loads(table, late + groups[g + 1], proj_weight, height)
        acc, loaded = preact_add([t for _, t in waiting], [weights[e] for e, _ in waiting if e in weights], acc, loads)
        keep(loads.events, loaded)
        waiting = []

    n_parts = 1
    last = event[-far]
    picks = ready_picks(far)
    pgs, back_sums, stats, made[last], picked = slopes(
        table, last, block[-far], weights[last], gain, bias, sums, acc, pbias, act_grad, n_parts,
        list(made.items()) if picks else [], picks,
    )
    send(picked)

    rights = []
    for pg in pgs:
        pieces = {0: pg}
        for k in plan.evens:
            pieces[k] = swap(pg, k)
        for k in [0, *plan.evens]:
            pieces[k + 1] = swap(pieces[k], 1)
        rights.append([pieces[k] for k in range(n_dp)])
    lefts = {}
    for k in [0, *plan.evens]:
        if k:
            arrived = [(a, j) for a in sent[k] for j in range(a.shape[0] // height)]
            candidates = [(i, a[j * height : (j + 1) * height]) for i, (a, j) in enumerate(arrived)]
            first = plan.column["sort"]
        else:
            candidates = list(made.items())
            first = plan.column["own"]
        mine, other = choose(table, list(range(first, first + 2 * per)), candidates, 2)
        lefts[k] = mine
        lefts[k + 1] = swap(other, 1)
    lefts = [lefts[k] for k in range(n_dp)]

    message = back_blocks([weights[last]], pgs, back_sums, [True])[0]
    up = along(message, 1)
    down = None
    for d in range(far - 1, 0, -1):
        first = down is None
        a, b = back_blocks([weights[event[d]], weights[event[-d]]], pgs, back_sums, [False, first])
        if not first:
            b = add_message(b, down, back_sums)
        down = along(b, -1)
        a = add_message(a, up, back_sums)
        up = along(a, 1)
    own, columns, centred = back_own(table, weights[0], pgs, inputs, gain, stats)
    got = [up] if down is None else [up, down]
    grad_inputs = finish(own, columns, centred, stats, got, back_sums, width)

    rows = lefts[0].shape[0]
    tiles = 6 if rows % (6 * 16) == 0 else 1
    cuts = [0, 0, tiles] if tiles > 0 > 0 else [0, tiles]
    grad_weight = None
    for span in zip(cuts, cuts[1:]):
        grad_weight = grad_part(lefts, rights[0], grad_weight, span, rows // tiles, factor)
    return (grad_inputs, grad_weight)


def solution(mesh):
    in_specs = (P("mp", "dp"), P(), P(), P(None, "mp"), P("mp"), P("dp", "mp"))
    out_specs = (P("mp", "dp"), P("dp", "mp"))

    return jax.shard_map(on_device, mesh=mesh, in_specs=in_specs, out_specs=out_specs, check_vma=False)
```

```python
import math

import jax
import jax.numpy as jnp
import numpy as np
from jax import lax
from jax.experimental import pallas as pl
from jax.experimental.pallas import tpu as pltpu
from jax.sharding import PartitionSpec as P


epsilon = 1e-06
root_half = 0.7071067811865476
density_norm = 0.3989422804014327
f32, bf16 = jnp.float32, jnp.bfloat16
VMEM_BYTES = 16 * 1024 * 1024
EXTRA = 16


def ring_of(size, columns):
    rows = size // columns
    if columns < 2 or rows < 2 or rows % 2 or size % columns:
        return list(range(size))
    walk = []
    for row in range(rows):
        inner = range(1, columns)
        walk += [row * columns + c for c in (inner if row % 2 == 0 else reversed(inner))]
    return walk + [row * columns for row in reversed(range(rows))]


def column_of(row):
    n = row.shape[1]
    step = 128 if n % 128 == 0 else n
    parts = [
        jnp.broadcast_to(row[:, i : i + step], (128, step)).T for i in range(0, n, step)
    ]
    return parts[0] if len(parts) == 1 else jnp.concatenate(parts, axis=0)


def row_of(column):
    return jnp.broadcast_to(column, (128, 128)).T[0:1, :]


def gelu_slope(preact):
    cumulative = 0.5 * (1.0 + lax.erf(preact * root_half))
    return cumulative + preact * density_norm * jnp.exp(-0.5 * preact * preact)


class Args:
    def __init__(self):
        self.values, self.specs = [], []

    def put(self, values, space=pltpu.VMEM):
        for value in values:
            self.values.append(value)
            self.specs.append(pl.BlockSpec(memory_space=space))
        return self


def run(body, args, outs, flops, moved, scratch=(), out_spaces=None, limit=VMEM_BYTES):
    spaces = out_spaces or [pltpu.VMEM] * len(outs)
    return pl.pallas_call(
        body,
        in_specs=args.specs,
        out_specs=[pl.BlockSpec(memory_space=s) for s in spaces],
        out_shape=outs,
        scratch_shapes=list(scratch),
        compiler_params=pltpu.CompilerParams(vmem_limit_bytes=limit),
        cost_estimate=pl.CostEstimate(
            flops=int(flops), bytes_accessed=int(moved), transcendentals=0
        ),
    )(*args.values)


shape_of = jax.ShapeDtypeStruct


def sums_of(xs):
    count, tokens = len(xs), xs[0].shape[1]

    def body(*refs):
        out = refs[-1]
        one = two = None
        for i, x_ref in enumerate(refs[:-1]):
            values = x_ref[...].astype(f32)
            a = jnp.sum(values, axis=0, keepdims=True)
            b = jnp.sum(values * values, axis=0, keepdims=True)
            out[2 * i : 2 * i + 1, :] = a
            out[2 * i + 1 : 2 * i + 2, :] = b
            one, two = (a, b) if one is None else (one + a, two + b)
        out[2 * count : 2 * count + 1, :] = one
        out[2 * count + 1 : 2 * count + 2, :] = two

    outs = [shape_of((2 * count + 2, tokens), f32)]
    return run(body, Args().put(xs), outs, 4e8, 10**6)[0]


def total_of(parts):
    one = two = None
    for ref, row in parts:
        a, b = ref[row : row + 1, :], ref[row + 1 : row + 2, :]
        one, two = (a, b) if one is None else (one + a, two + b)
    return one, two


def split(one, two):
    terms = []
    for v in (one, two):
        high = v.astype(bf16).astype(f32)
        terms += [high, v - high]
    terms.append(jnp.zeros((EXTRA - 4, one.shape[1]), f32))
    return jnp.concatenate(terms, axis=0).astype(bf16)


def merge(ref, height):
    rows = ref[height : height + EXTRA, :].astype(f32)
    return rows[0:1, :] + rows[1:2, :], rows[2:3, :] + rows[3:4, :]


class Loads:
    def __init__(self, table, events, weight, height):
        self.table, self.events, self.weight, self.height = table, events, weight, height
        self.outs = [pltpu.VMEM((height, weight.shape[1]), bf16)] * len(events)

    def copies(self, table_ref, w_ref, outs, sem):
        made = []
        for i, e in enumerate(self.events):
            at = pl.multiple_of(table_ref[0, e] * self.height, self.height)
            made.append(
                pltpu.make_async_copy(w_ref.at[pl.ds(at, self.height), :], outs[i], sem.at[i])
            )
        return made

    @property
    def scratch(self):
        return [pltpu.SemaphoreType.DMA((max(len(self.events), 1),))]


def load_blocks(loads):
    def body(table_ref, w_ref, *refs):
        copies = loads.copies(table_ref, w_ref, refs[:-1], refs[-1])
        for c in copies:
            c.start()
        for c in copies:
            c.wait()

    args = Args().put([loads.table], pltpu.SMEM).put([loads.weight], pl.ANY)
    return run(body, args, loads.outs, 1e8, 10**6, loads.scratch)


def normalize(x, g, b, average, inv_std):
    centred = (x.astype(f32) - average) * inv_std
    return centred * column_of(g) + column_of(b)


def turn(normed, g, b, tokens, out):
    out[0:tokens, :] = normed.T.astype(bf16)
    out[tokens : tokens + EXTRA, :] = split(g, b)


def chunk_of(n, most):
    for parts in range(1, n + 1):
        if n % parts == 0 and n // parts <= most and (n // parts) % 128 == 0:
            return n // parts
    return n


def stats_of(sum_refs, sum_rows, width):
    one, two = total_of(list(zip(sum_refs, sum_rows)))
    average = one / width
    return average, lax.rsqrt(two / width - average * average + epsilon)


def stage(table, events, xs, weights, gain, bias, sums, acc, loads):
    count, (height, tokens) = len(xs), xs[0].shape
    hidden = weights[0].shape[1]
    width = height * gain.shape[0]
    step = chunk_of(hidden, 1024)
    sum_arrays, sum_rows = [v for v, _ in sums], [r for _, r in sums]
    n_loads, n_sums = len(loads.events), len(sums)

    def body(table_ref, w_any, gain_ref, bias_ref, *refs):
        refs = list(refs)
        take = lambda n: [refs.pop(0) for _ in range(n)]
        x_refs, w_refs, sum_refs = take(count), take(count), take(n_sums)
        acc_ref = take(1)[0] if acc is not None else None
        straight, out, loaded, turned, sem = take(count), take(1)[0], take(n_loads), take(count), take(1)[0]
        copies = loads.copies(table_ref, w_any, loaded, sem)
        for c in copies:
            c.start()
        average, inv_std = stats_of(sum_refs, sum_rows, width)
        for i, e in enumerate(events):
            g, b = gain_ref[table_ref[0, e]], bias_ref[table_ref[0, e]]
            normed = normalize(x_refs[i][...], g, b, average, inv_std)
            straight[i][...] = normed.astype(bf16)
            turn(normed, g, b, tokens, turned[i])

        def one(j, _):
            at = pl.ds(pl.multiple_of(j * step, step), step)
            total = acc_ref[:, at] if acc is not None else None
            for t, w in zip(turned, w_refs):
                term = jnp.dot(t[...], w[:, at], preferred_element_type=f32)
                total = term if total is None else total + term
            out[:, at] = total
            return 0

        lax.fori_loop(0, hidden // step, one, 0)
        for c in copies:
            c.wait()

    args = Args().put([table], pltpu.SMEM).put([loads.weight], pl.ANY).put([gain, bias])
    args.put(xs).put(weights).put(sum_arrays)
    if acc is not None:
        args.put([acc])
    outs = [shape_of((height, tokens), bf16)] * count
    outs += [shape_of((tokens + EXTRA, hidden), f32)] + loads.outs
    made = run(
        body, args, outs, 2e8 * count, 10**6,
        [pltpu.VMEM((tokens + EXTRA, height), bf16)] * count + loads.scratch,
    )
    return made[:count], made[count], made[count + 1 :]


def slopes(table, event, x, weight, gain, bias, sums, acc, pbias, act, n_parts):
    height, tokens = x.shape
    hidden = weight.shape[1]
    width = height * gain.shape[0]
    wide = hidden // n_parts
    step = chunk_of(wide, 512)
    sum_arrays, sum_rows = [v for v, _ in sums], [r for _, r in sums]

    def body(table_ref, gain_ref, bias_ref, x_ref, w_ref, acc_ref, pbias_ref, act_ref, *refs):
        refs = list(refs)
        sum_refs = [refs.pop(0) for _ in sums]
        outs = [refs.pop(0) for _ in range(n_parts)]
        sums_out, stats, straight, turned = refs
        average, inv_std = stats_of(sum_refs, sum_rows, width)
        stats[0:1, :] = average
        stats[1:2, :] = inv_std
        g, b = gain_ref[table_ref[0, event]], bias_ref[table_ref[0, event]]
        normed = normalize(x_ref[...], g, b, average, inv_std)
        straight[...] = normed.astype(bf16)
        turn(normed, g, b, tokens, turned)
        one_sum = two_sum = jnp.zeros((tokens, 1), f32)
        for part, out in enumerate(outs):

            def one(j, carry, part=part, out=out):
                one_sum, two_sum = carry
                here = pl.ds(pl.multiple_of(part * wide + j * step, step), step)
                total = acc_ref[:, here] + jnp.dot(
                    turned[...], w_ref[:, here], preferred_element_type=f32
                )
                inner = total[0:tokens, :]
                gain_sum = total[tokens : tokens + 1, :] + total[tokens + 1 : tokens + 2, :]
                bias_sum = total[tokens + 2 : tokens + 3, :] + total[tokens + 3 : tokens + 4, :]
                slope = gelu_slope(inner + pbias_ref[:, here])
                grad = (act_ref[:, here].astype(f32) * slope).astype(bf16)
                out[:, pl.ds(pl.multiple_of(j * step, step), step)] = grad
                wide_grad = grad.astype(f32)
                one_sum = one_sum + jnp.sum(wide_grad * gain_sum, axis=1, keepdims=True)
                two_sum = two_sum + jnp.sum(wide_grad * (inner - bias_sum), axis=1, keepdims=True)
                return one_sum, two_sum

            one_sum, two_sum = lax.fori_loop(0, wide // step, one, (one_sum, two_sum))
        sums_out[0:1, :] = row_of(one_sum)
        sums_out[1:2, :] = row_of(two_sum)

    args = Args().put([table], pltpu.SMEM).put([gain, bias, x, weight, acc, pbias, act]).put(sum_arrays)
    outs = [shape_of((tokens, wide), bf16)] * n_parts + [shape_of((2, tokens), f32)] * 2
    outs += [shape_of((height, tokens), bf16)]
    made = run(body, args, outs, 8e8, 10**6, [pltpu.VMEM((tokens + EXTRA, height), bf16)])
    return made[:n_parts], made[n_parts], made[n_parts + 1], made[n_parts + 2]


def back_blocks(weights, pgs, sums, as_message):
    count, height, tokens = len(weights), weights[0].shape[0], pgs[0].shape[0]
    step = 256 if height % 256 == 0 else height

    def body(sums_ref, *refs):
        w_refs, pg_refs, outs = refs[:count], refs[count : count + len(pgs)], refs[count + len(pgs) :]

        def one(j, _):
            at = pl.ds(pl.multiple_of(j * step, step), step)
            for w, out in zip(w_refs, outs):
                total, column = None, 0
                for pg in pg_refs:
                    wide = pg.shape[1]
                    term = lax.dot_general(
                        w[at, column : column + wide], pg[...], (((1,), (1,)), ((), ())),
                        preferred_element_type=f32,
                    )
                    total = term if total is None else total + term
                    column += wide
                out[at, :] = total.astype(out.dtype)
            return 0

        lax.fori_loop(0, height // step, one, 0)
        for i in range(count):
            if as_message[i]:
                outs[i][height : height + EXTRA, :] = split(sums_ref[0:1, :], sums_ref[1:2, :])

    args = Args().put([sums]).put(weights).put(pgs)
    outs = [
        shape_of((height + EXTRA, tokens), bf16) if m else shape_of((height, tokens), f32)
        for m in as_message
    ]
    return run(body, args, outs, 2e8 * count, 10**6)


def add_message(part, got, sums):
    height, _ = part.shape

    def body(part_ref, got_ref, sums_ref, out):
        out[0:height, :] = (part_ref[...] + got_ref[0:height, :].astype(f32)).astype(bf16)
        one, two = merge(got_ref, height)
        out[height : height + EXTRA, :] = split(one + sums_ref[0:1, :], two + sums_ref[1:2, :])

    args = Args().put([part, got, sums])
    return run(body, args, [shape_of(got.shape, bf16)], 1e8, 10**6)[0]


def choose(table, columns, candidates, count_of=1):
    labels = [label for label, _ in candidates]
    arrays = [array for _, array in candidates]
    height, tokens = arrays[0].shape[-2:]

    def body(table_ref, *refs):
        inputs, outs = refs[: len(arrays)], refs[len(arrays) :]
        for i, column in enumerate(columns):
            wanted = table_ref[0, column]
            for label, ref in zip(labels, inputs):

                @pl.when(wanted == label)
                def _(ref=ref, i=i):
                    at = (i % (len(columns) // count_of)) * height
                    outs[i // (len(columns) // count_of)][at : at + height, :] = ref[...]

    args = Args().put([table], pltpu.SMEM).put(arrays)
    outs = [shape_of((len(columns) // count_of * height, tokens), bf16)] * count_of
    return run(body, args, outs, 2e8, 10**6)


def finish(table, x, gain, stats, own, got, sums):
    height, _ = x.shape
    width = height * gain.shape[0]

    def body(table_ref, x_ref, gain_ref, stats_ref, own_ref, sums_ref, *refs):
        out = refs[-1]
        one, two = sums_ref[0:1, :], sums_ref[1:2, :]
        grad = own_ref[...]
        for g in refs[:-1]:
            grad = grad + g[0:height, :].astype(f32)
            a, b = merge(g, height)
            one, two = one + a, two + b
        first_term, second_term = one / width, two / width
        average, inv_std = stats_ref[0:1, :], stats_ref[1:2, :]
        scaled = grad * column_of(gain_ref[table_ref[0, 0]])
        centred = (x_ref[...].astype(f32) - average) * inv_std
        out[...] = (inv_std * (scaled - first_term - centred * second_term)).astype(bf16)

    args = Args().put([table], pltpu.SMEM).put([x, gain, stats, own, sums]).put(got)
    return run(body, args, [shape_of(x.shape, bf16)], 3e8, 10**6)[0]


def grad_part(lefts, rights, target, at, total_columns, factor):
    count = len(lefts)
    height, tokens = lefts[0].shape
    columns = rights[0].shape[1]
    tiles = 3 if height % (3 * 128) == 0 else 1
    tile = height // tiles

    def body(*refs):
        refs = list(refs)
        left_refs, right_refs = refs[:count], refs[count : 2 * count]
        out, joined = refs[-2:]

        @pl.when(pl.program_id(0) == 0)
        def _():
            for k in range(count):
                joined[k * tokens : (k + 1) * tokens, :] = right_refs[k][...]

        left = jnp.concatenate([l[...] for l in left_refs], axis=1)
        out[...] = jnp.dot(left, joined[...], preferred_element_type=f32) * factor

    specs = [pl.BlockSpec((tile, tokens), lambda i: (i, 0)) for _ in lefts]
    specs += [pl.BlockSpec((tokens, columns), lambda i: (0, 0)) for _ in rights]
    args = [*lefts, *rights]
    aliases = {}
    if target is not None:
        aliases = {len(args): 0}
        args.append(target)
        specs.append(pl.BlockSpec(memory_space=pl.ANY))
    return pl.pallas_call(
        body,
        grid=(tiles,),
        in_specs=specs,
        out_specs=pl.BlockSpec((tile, columns), lambda i: (i, at)),
        out_shape=shape_of((height, total_columns), f32),
        scratch_shapes=[pltpu.VMEM((count * tokens, columns), bf16)],
        input_output_aliases=aliases,
        compiler_params=pltpu.CompilerParams(vmem_limit_bytes=VMEM_BYTES),
        cost_estimate=pl.CostEstimate(
            flops=int(5e8), bytes_accessed=height * columns * 4, transcendentals=0
        ),
        name="weight_grad",
    )(*args)


class Plan:
    def __init__(self, n_mp, n_dp):
        ring = ring_of(n_mp, max(n_dp // 2, 1))
        place = {m: i for i, m in enumerate(ring)}
        self.ring = ring
        self.far = far = n_mp // 2
        self.shifts = [0] + [s for d in range(1, far) for s in (-d, d)] + [-far]
        self.event = {s: i for i, s in enumerate(self.shifts)}
        self.per = per = n_mp // n_dp
        block_at = [[ring[(place[m] + s) % n_mp] for s in self.shifts] for m in range(n_mp)]
        event_of = [{b: e for e, b in enumerate(row)} for row in block_at]

        def slots(m, p):
            first = p // 2 * 2 * per
            return sorted(event_of[m][b] for b in range(first, first + 2 * per))

        self.evens = list(range(2, n_dp, 2))
        self.slot_step = [
            max(abs(self.shifts[slots(m, p)[j]]) for m in range(n_mp) for p in range(n_dp))
            for j in range(2 * per)
        ]
        rows = []
        self.column = {}
        for m in range(n_mp):
            for p in range(n_dp):
                row = list(block_at[m])
                for k in self.evens:
                    self.column["send", k] = len(row)
                    row += slots(m, p ^ k)
                mine = [p * per + i for i in range(per)] + [(p ^ 1) * per + i for i in range(per)]
                self.column["own"] = len(row)
                row += [event_of[m][b] for b in mine]
                self.column["sort"] = len(row)
                order = slots(m, p)
                row += [order.index(event_of[m][b]) for b in mine]
                rows.append(row)
        self.table = np.array(rows, np.int32).reshape(n_mp * n_dp, 1, -1)


def on_device(inputs, norm_gain, norm_bias, proj_weight, proj_bias, act_grad):
    height, tokens = inputs.shape
    hidden = proj_weight.shape[1]
    n_mp, n_dp = lax.axis_size("mp"), lax.axis_size("dp")
    factor = 1.0 / math.sqrt(tokens * n_dp)
    plan = Plan(n_mp, n_dp)
    far, per, shifts, event = plan.far, plan.per, plan.shifts, plan.event
    table = lax.dynamic_index_in_dim(
        jnp.asarray(plan.table), lax.axis_index("mp") * n_dp + lax.axis_index("dp"), 0, keepdims=False
    )
    gain = norm_gain.reshape(n_mp, 1, height)
    bias = norm_bias.reshape(n_mp, 1, height)
    pbias = proj_bias.reshape(1, hidden)

    def swap(value, k):
        return lax.ppermute(value, "dp", [(i, i ^ k) for i in range(n_dp)])

    def along(value, steps):
        pairs = [(plan.ring[i], plan.ring[(i + steps) % n_mp]) for i in range(n_mp)]
        return lax.ppermute(value, "mp", pairs)

    block = {0: inputs}
    for d in range(1, far + 1):
        block[-d] = along(block[-d + 1], 1)
        if d < far:
            block[d] = along(block[d - 1], -1)

    groups = [[0]] + [[event[-d], event[d]] for d in range(1, far)] + [[event[-far]]]
    if far > 1:
        groups[:2] = [groups[0] + groups[1]]
    if far == 4:
        window = sums_of([block[0], block[-1], block[1]])
        below = along(window, 3)
        above = along(window, -3)
        sums = [(window, 6), (below, 6), (above, 0), (above, 2)]
    else:
        total, k = sums_of([inputs])[0:2], 1
        while k < n_mp:
            total = total + lax.ppermute(total, "mp", [(i, i ^ k) for i in range(n_mp)])
            k *= 2
        sums = [(total, 0)]

    weights, made = {}, {}

    def keep(events, arrays):
        for e, w in zip(events, arrays):
            weights[e] = pltpu.with_memory_space_constraint(w, pltpu.VMEM)

    keep(groups[0], load_blocks(Loads(table, groups[0], proj_weight, height)))
    acc, sent, slot = None, {k: [] for k in plan.evens}, 0

    def send_ready(reach):
        nonlocal slot
        more = sum(1 for s in plan.slot_step[slot:] if s <= reach)
        if more:
            for k in plan.evens:
                first = plan.column["send", k] + slot
                picked = choose(table, list(range(first, first + more)), list(made.items()))[0]
                sent[k].append(swap(picked, k))
            slot += more

    for g, events in enumerate(groups[:-1]):
        reach = max(abs(shifts[e]) for e in events)
        loads = Loads(table, groups[g + 1], proj_weight, height)
        straight, acc, loaded = stage(
            table, events, [block[shifts[e]] for e in events], [weights[e] for e in events],
            gain, bias, sums, acc, loads,
        )
        keep(loads.events, loaded)
        made.update(zip(events, straight))
        send_ready(reach)

    n_parts = 2 if hidden % 1024 == 0 else 1
    last = event[-far]
    pgs, back_sums, stats, made[last] = slopes(
        table, last, block[-far], weights[last], gain, bias, sums, acc, pbias, act_grad, n_parts
    )
    send_ready(far)

    rights = []
    for pg in pgs:
        pieces = {0: pg}
        for k in plan.evens:
            pieces[k] = swap(pg, k)
        for k in [0, *plan.evens]:
            pieces[k + 1] = swap(pieces[k], 1)
        rights.append([pieces[k] for k in range(n_dp)])
    lefts = {}
    for k in [0, *plan.evens]:
        if k:
            arrived = [(a, j) for a in sent[k] for j in range(a.shape[0] // height)]
            candidates = [(i, a[j * height : (j + 1) * height]) for i, (a, j) in enumerate(arrived)]
            first = plan.column["sort"]
        else:
            candidates = list(made.items())
            first = plan.column["own"]
        mine, other = choose(table, list(range(first, first + 2 * per)), candidates, 2)
        lefts[k] = mine
        lefts[k + 1] = swap(other, 1)
    lefts = [lefts[k] for k in range(n_dp)]

    message = back_blocks([weights[last]], pgs, back_sums, [True])[0]
    up = along(message, 1)
    down = None
    for d in range(far - 1, 0, -1):
        first = down is None
        a, b = back_blocks([weights[event[d]], weights[event[-d]]], pgs, back_sums, [False, first])
        if not first:
            b = add_message(b, down, back_sums)
        down = along(b, -1)
        a = add_message(a, up, back_sums)
        up = along(a, 1)
    own = back_blocks([weights[0]], pgs, back_sums, [False])[0]
    got = [up] if down is None else [up, down]
    grad_inputs = finish(table, inputs, gain, stats, own, got, back_sums)

    grad_weight = None
    for at, right in enumerate(rights):
        grad_weight = grad_part(lefts, right, grad_weight, at, hidden, factor)
    return (grad_inputs, grad_weight)


def solution(mesh):
    in_specs = (P("mp", "dp"), P(), P(), P(None, "mp"), P("mp"), P("dp", "mp"))
    out_specs = (P("mp", "dp"), P("dp", "mp"))

    return jax.shard_map(on_device, mesh=mesh, in_specs=in_specs, out_specs=out_specs, check_vma=False)
```

```python
import math

import jax
import jax.numpy as jnp
import numpy as np
from jax import lax
from jax.experimental import pallas as pl
from jax.experimental.pallas import tpu as pltpu
from jax.sharding import PartitionSpec as P


epsilon = 1e-06
root_half = 0.7071067811865476
density_norm = 0.3989422804014327
f32, bf16 = jnp.float32, jnp.bfloat16
VMEM_BYTES = 8 * 1024 * 1024
PIECES = 1
EXTRA = 16


def ring_of(size, columns):
    rows = size // columns
    if columns < 2 or rows < 2 or rows % 2 or size % columns:
        return list(range(size))
    walk = []
    for row in range(rows):
        inner = range(1, columns)
        walk += [row * columns + c for c in (inner if row % 2 == 0 else reversed(inner))]
    return walk + [row * columns for row in reversed(range(rows))]


def column_of(row, tokens):
    n = row.shape[1]
    step = 128 if n % 128 == 0 else n
    parts = [
        jnp.broadcast_to(row[:, i : i + step], (tokens, step)).T for i in range(0, n, step)
    ]
    return parts[0] if len(parts) == 1 else jnp.concatenate(parts, axis=0)


def row_of(column):
    return jnp.broadcast_to(column, (column.shape[0], column.shape[0])).T[0:1, :]


def gelu_slope(preact):
    cumulative = 0.5 * (1.0 + lax.erf(preact * root_half))
    return cumulative + preact * density_norm * jnp.exp(-0.5 * preact * preact)


class Args:
    def __init__(self):
        self.values, self.specs = [], []

    def put(self, values, space=pltpu.VMEM):
        for value in values:
            self.values.append(value)
            self.specs.append(pl.BlockSpec(memory_space=space))
        return self


def run(body, args, outs, flops, moved, scratch=(), out_spaces=None, limit=VMEM_BYTES):
    spaces = out_spaces or [pltpu.VMEM] * len(outs)
    return pl.pallas_call(
        body,
        in_specs=args.specs,
        out_specs=[pl.BlockSpec(memory_space=s) for s in spaces],
        out_shape=outs,
        scratch_shapes=list(scratch),
        compiler_params=pltpu.CompilerParams(vmem_limit_bytes=limit),
        cost_estimate=pl.CostEstimate(
            flops=int(flops), bytes_accessed=int(moved), transcendentals=0
        ),
    )(*args.values)


shape_of = jax.ShapeDtypeStruct


def sums_of(xs):
    count, tokens = len(xs), xs[0].shape[1]

    def body(*refs):
        out = refs[-1]
        one = two = None
        for i, x_ref in enumerate(refs[:-1]):
            values = x_ref[...].astype(f32)
            a = jnp.sum(values, axis=0, keepdims=True)
            b = jnp.sum(values * values, axis=0, keepdims=True)
            out[2 * i : 2 * i + 1, :] = a
            out[2 * i + 1 : 2 * i + 2, :] = b
            one, two = (a, b) if one is None else (one + a, two + b)
        out[2 * count : 2 * count + 1, :] = one
        out[2 * count + 1 : 2 * count + 2, :] = two

    outs = [shape_of((2 * count + 2, tokens), f32)]
    return run(body, Args().put(xs), outs, 4e8, 10**6)[0]


def total_of(parts):
    one = two = None
    for ref, row in parts:
        a, b = ref[row : row + 1, :], ref[row + 1 : row + 2, :]
        one, two = (a, b) if one is None else (one + a, two + b)
    return one, two


def split(one, two):
    terms = []
    for v in (one, two):
        high = v.astype(bf16).astype(f32)
        terms += [high, v - high]
    terms.append(jnp.zeros((EXTRA - 4, one.shape[1]), f32))
    return jnp.concatenate(terms, axis=0).astype(bf16)


def merge(ref, height):
    rows = ref[height : height + EXTRA, :].astype(f32)
    return rows[0:1, :] + rows[1:2, :], rows[2:3, :] + rows[3:4, :]


class Loads:
    def __init__(self, table, events, weight, height):
        self.table, self.events, self.weight, self.height = table, events, weight, height
        self.outs = [pltpu.VMEM((height, weight.shape[1]), bf16)] * len(events)

    def copies(self, table_ref, w_ref, outs, sem):
        made, piece = [], self.height // PIECES
        for i, e in enumerate(self.events):
            for j in range(PIECES):
                at = pl.multiple_of(table_ref[0, e] * self.height + j * piece, piece)
                made.append(
                    pltpu.make_async_copy(
                        w_ref.at[pl.ds(at, piece), :], outs[i].at[j * piece : (j + 1) * piece, :],
                        sem.at[i * PIECES + j],
                    )
                )
        return made

    @property
    def scratch(self):
        return [pltpu.SemaphoreType.DMA((max(len(self.events), 1) * PIECES,))]


def load_blocks(loads):
    def body(table_ref, w_ref, *refs):
        copies = loads.copies(table_ref, w_ref, refs[:-1], refs[-1])
        for c in copies:
            c.start()
        for c in copies:
            c.wait()

    args = Args().put([loads.table], pltpu.SMEM).put([loads.weight], pltpu.HBM)
    return run(body, args, loads.outs, 1e8, 10**6, loads.scratch, limit=8 * 1024 * 1024)


def normalize(x_ref, g, b, average, inv_std, straight, turned):
    tokens = x_ref.shape[1]
    centred = (x_ref[...].T.astype(f32) - average) * inv_std
    normed = (centred * g + b).astype(bf16)
    turned[0:tokens, :] = normed
    turned[tokens : tokens + EXTRA, :] = split(g, b)
    straight[...] = normed.T


def chunk_of(n, most):
    for parts in range(1, n + 1):
        if n % parts == 0 and n // parts <= most and (n // parts) % 128 == 0:
            return n // parts
    return n


def stats_of(refs, rows, width):
    one, two = total_of(list(zip(refs, rows)))
    average = one / width
    return average, lax.rsqrt(two / width - average * average + epsilon)


def stats_columns(average, inv_std):
    return tuple(jnp.broadcast_to(v, (128, v.shape[1])).T[:, 0:1] for v in (average, inv_std))


def pick(table_ref, columns, labels, refs, out, height):
    for i, column in enumerate(columns):
        wanted = table_ref[0, column]
        for label, ref in zip(labels, refs):

            @pl.when(wanted == label)
            def _(ref=ref, i=i):
                out[i * height : (i + 1) * height, :] = ref[...]


def norm_blocks(table, events, xs, gain, bias, sums, pool, picks):
    count, (height, tokens) = len(xs), xs[0].shape
    width = height * gain.shape[0]
    sum_arrays, sum_rows = [v for v, _ in sums], [r for _, r in sums]
    labels = [e for e, _ in pool] + list(events)

    def body(table_ref, gain_ref, bias_ref, *refs):
        refs = list(refs)
        take = lambda n: [refs.pop(0) for _ in range(n)]
        x_refs, sum_refs, pool_refs = take(count), take(len(sums)), take(len(pool))
        straight, turned, picked = take(count), take(count), refs
        columns = stats_columns(*stats_of(sum_refs, sum_rows, width))
        for i, e in enumerate(events):
            g, b = gain_ref[table_ref[0, e]], bias_ref[table_ref[0, e]]
            normalize(x_refs[i], g, b, *columns, straight[i], turned[i])
        for wanted, target in zip(picks, picked):
            pick(table_ref, wanted, labels, pool_refs + straight, target, height)

    args = Args().put([table], pltpu.SMEM).put([gain, bias]).put(xs).put(sum_arrays)
    args.put([array for _, array in pool])
    outs = [shape_of((height, tokens), bf16)] * count
    outs += [shape_of((tokens + EXTRA, height), bf16)] * count
    outs += [shape_of((len(wanted) * height, tokens), bf16) for wanted in picks]
    made = run(body, args, outs, 1e8 * count, 10**6)
    return made[:count], made[count : 2 * count], made[2 * count :]


def preact_add(turned, weights, acc, loads):
    count, ready = len(turned), len(weights)
    late = count - ready
    rows = turned[0].shape[0]
    hidden = loads.weight.shape[1]
    step = chunk_of(hidden, 1536 if count > 2 else 1024)
    n_loads = len(loads.events)

    def body(table_ref, w_any, *refs):
        refs = list(refs)
        take = lambda n: [refs.pop(0) for _ in range(n)]
        t_refs, w_refs = take(count), take(ready)
        acc_ref = take(1)[0] if acc is not None else None
        out, loaded, sem = take(1)[0], take(n_loads), refs[0]
        copies = loads.copies(table_ref, w_any, loaded, sem)
        for c in copies:
            c.start()

        def add(pairs, base):
            def one(j, _):
                at = pl.ds(pl.multiple_of(j * step, step), step)
                total = base[:, at] if base is not None else None
                for t, w in pairs:
                    term = jnp.dot(t[...], w[:, at], preferred_element_type=f32)
                    total = term if total is None else total + term
                out[:, at] = total
                return 0

            lax.fori_loop(0, hidden // step, one, 0, unroll=len(pairs) <= 2)

        if ready:
            add(list(zip(t_refs, w_refs)), acc_ref)
        for c in copies[: late * PIECES]:
            c.wait()
        if late:
            add(list(zip(t_refs[ready:], loaded)), out if ready else acc_ref)
        for c in copies[late * PIECES :]:
            c.wait()

    args = Args().put([loads.table], pltpu.SMEM).put([loads.weight], pltpu.HBM).put(turned).put(weights)
    if acc is not None:
        args.put([acc])
    outs = [shape_of((rows, hidden), f32)] + loads.outs
    made = run(body, args, outs, 2e8 * count, 10**6, loads.scratch)
    return made[0], made[1:]


def slopes(table, event, x, weight, gain, bias, sums, acc, pbias, act, n_parts, pool, picks):
    height, tokens = x.shape
    hidden = weight.shape[1]
    width = height * gain.shape[0]
    wide = hidden // n_parts
    step = chunk_of(wide, 512)
    labels = [e for e, _ in pool] + [event]
    sum_arrays, sum_rows = [v for v, _ in sums], [r for _, r in sums]

    def body(table_ref, gain_ref, bias_ref, x_ref, w_ref, acc_ref, pbias_ref, act_ref, *refs):
        refs = list(refs)
        take = lambda n: [refs.pop(0) for _ in range(n)]
        sum_refs, pool_refs, outs = take(len(sums)), take(len(pool)), take(n_parts)
        sums_out, stats, straight = take(3)
        picked, turned = take(len(picks)), refs[0]
        average, inv_std = stats_of(sum_refs, sum_rows, width)
        stats[0:1, :] = average
        stats[1:2, :] = inv_std
        g, b = gain_ref[table_ref[0, event]], bias_ref[table_ref[0, event]]
        normalize(x_ref, g, b, *stats_columns(average, inv_std), straight, turned)
        for wanted, target in zip(picks, picked):
            pick(table_ref, wanted, labels, pool_refs + [straight], target, height)
        one_sum = two_sum = jnp.zeros((tokens, 1), f32)
        for part, out in enumerate(outs):

            def one(j, carry, part=part, out=out):
                one_sum, two_sum = carry
                here = pl.ds(pl.multiple_of(part * wide + j * step, step), step)
                total = acc_ref[:, here] + jnp.dot(
                    turned[...], w_ref[:, here], preferred_element_type=f32
                )
                inner = total[0:tokens, :]
                gain_sum = total[tokens : tokens + 1, :] + total[tokens + 1 : tokens + 2, :]
                bias_sum = total[tokens + 2 : tokens + 3, :] + total[tokens + 3 : tokens + 4, :]
                slope = gelu_slope(inner + pbias_ref[:, here])
                grad = (act_ref[:, here].astype(f32) * slope).astype(bf16)
                out[:, pl.ds(pl.multiple_of(j * step, step), step)] = grad
                wide_grad = grad.astype(f32)
                one_sum = one_sum + jnp.sum(wide_grad * gain_sum, axis=1, keepdims=True)
                two_sum = two_sum + jnp.sum(wide_grad * (inner - bias_sum), axis=1, keepdims=True)
                return one_sum, two_sum

            one_sum, two_sum = lax.fori_loop(0, wide // step, one, (one_sum, two_sum), unroll=True)
        sums_out[0:1, :] = row_of(one_sum)
        sums_out[1:2, :] = row_of(two_sum)

    args = Args().put([table], pltpu.SMEM).put([gain, bias, x, weight, acc, pbias, act]).put(sum_arrays)
    args.put([array for _, array in pool])
    outs = [shape_of((tokens, wide), bf16)] * n_parts + [shape_of((2, tokens), f32)] * 2
    outs += [shape_of((height, tokens), bf16)]
    outs += [shape_of((len(wanted) * height, tokens), bf16) for wanted in picks]
    made = run(body, args, outs, 8e8, 10**6, [pltpu.VMEM((tokens + EXTRA, height), bf16)])
    return made[:n_parts], made[n_parts], made[n_parts + 1], made[n_parts + 2], made[n_parts + 3 :]


def back_blocks(weights, pgs, sums, as_message):
    count, height, tokens = len(weights), weights[0].shape[0], pgs[0].shape[0]
    step = 256 if height % 256 == 0 else height

    def body(sums_ref, *refs):
        w_refs, pg_refs, outs = refs[:count], refs[count : count + len(pgs)], refs[count + len(pgs) :]

        def one(j, _):
            at = pl.ds(pl.multiple_of(j * step, step), step)
            for w, out in zip(w_refs, outs):
                total, column = None, 0
                for pg in pg_refs:
                    wide = pg.shape[1]
                    term = lax.dot_general(
                        w[at, column : column + wide], pg[...], (((1,), (1,)), ((), ())),
                        preferred_element_type=f32,
                    )
                    total = term if total is None else total + term
                    column += wide
                out[at, :] = total.astype(out.dtype)
            return 0

        lax.fori_loop(0, height // step, one, 0, unroll=True)
        for i in range(count):
            if as_message[i]:
                outs[i][height : height + EXTRA, :] = split(sums_ref[0:1, :], sums_ref[1:2, :])

    args = Args().put([sums]).put(weights).put(pgs)
    outs = [
        shape_of((height + EXTRA, tokens), bf16) if m else shape_of((height, tokens), f32)
        for m in as_message
    ]
    return run(body, args, outs, 2e8 * count, 10**6)


def add_message(part, got, sums):
    height, _ = part.shape

    def body(part_ref, got_ref, sums_ref, out):
        out[0:height, :] = (part_ref[...] + got_ref[0:height, :].astype(f32)).astype(bf16)
        one, two = merge(got_ref, height)
        out[height : height + EXTRA, :] = split(one + sums_ref[0:1, :], two + sums_ref[1:2, :])

    args = Args().put([part, got, sums])
    return run(body, args, [shape_of(got.shape, bf16)], 1e8, 10**6)[0]


def choose(table, columns, candidates, count_of=1):
    labels = [label for label, _ in candidates]
    arrays = [array for _, array in candidates]
    height, tokens = arrays[0].shape[-2:]

    def body(table_ref, *refs):
        inputs, outs = refs[: len(arrays)], refs[len(arrays) :]
        for i, column in enumerate(columns):
            wanted = table_ref[0, column]
            for label, ref in zip(labels, inputs):

                @pl.when(wanted == label)
                def _(ref=ref, i=i):
                    at = (i % (len(columns) // count_of)) * height
                    outs[i // (len(columns) // count_of)][at : at + height, :] = ref[...]

    args = Args().put([table], pltpu.SMEM).put(arrays)
    outs = [shape_of((len(columns) // count_of * height, tokens), bf16)] * count_of
    return run(body, args, outs, 2e8, 10**6)


def back_own(table, weight, pgs, x, gain, stats):
    height, tokens = x.shape

    def body(table_ref, w_ref, x_ref, gain_ref, stats_ref, *refs):
        pg_refs, (own, columns, centred) = refs[: len(pgs)], refs[len(pgs) :]
        total, at = None, 0
        for pg in pg_refs:
            term = lax.dot_general(
                w_ref[:, at : at + pg.shape[1]], pg[...], (((1,), (1,)), ((), ())),
                preferred_element_type=f32,
            )
            total = term if total is None else total + term
            at += pg.shape[1]
        own[...] = total
        columns[...] = column_of(gain_ref[table_ref[0, 0]], tokens)
        centred[...] = (x_ref[...].astype(f32) - stats_ref[0:1, :]) * stats_ref[1:2, :]

    args = Args().put([table], pltpu.SMEM).put([weight, x, gain, stats]).put(pgs)
    return run(body, args, [shape_of((height, tokens), f32)] * 3, 3e8, 10**6)


def finish(own_ref, columns_ref, centred_ref, stats_ref, sums_ref, got_refs, out, width):
    height = own_ref.shape[0]
    one, two = sums_ref[0:1, :], sums_ref[1:2, :]
    grad = own_ref[...]
    for g in got_refs:
        grad = grad + g[0:height, :].astype(f32)
        a, b = merge(g, height)
        one, two = one + a, two + b
    first_term, second_term = one / width, two / width
    scaled = grad * columns_ref[...]
    out[...] = (stats_ref[1:2, :] * (scaled - first_term - centred_ref[...] * second_term)).astype(bf16)


def grad_part(lefts, rights, target, span, tile, factor, ending=None):
    count = len(lefts)
    height, tokens = lefts[0].shape
    columns = rights[0].shape[1]
    n_tiles = span[1] - span[0]
    slots = min(6, n_tiles)

    def body(*refs):
        refs = list(refs)
        left_refs, right_refs = refs[:count], refs[count : 2 * count]
        if ending is None:
            out, joined, made, sem = refs[-4:]
        else:
            out, input_out, joined, made, sem, ended, ended_sem = refs[-7:]
            ended_copy = pltpu.make_async_copy(ended, input_out, ended_sem)
        for k in range(count):
            joined[k * tokens : (k + 1) * tokens, :] = right_refs[k][...]
        copies = []
        for i in range(n_tiles):
            at = slice((span[0] + i) * tile, (span[0] + i + 1) * tile)
            slot = i % slots
            if i >= slots:
                copies[i - slots].wait()
            left = jnp.concatenate([l[at, :] for l in left_refs], axis=1)
            made[slot] = jnp.dot(left, joined[...], preferred_element_type=f32) * factor
            copies.append(pltpu.make_async_copy(made.at[slot], out.at[at, :], sem.at[slot]))
            copies[-1].start()
            if i == 0 and ending is not None:
                given = refs[len(args) - len(ending_args) : len(args)]
                finish(*given[:5], given[5:], ended, ending_width)
                ended_copy.start()
        if ending is not None:
            ended_copy.wait()
        for c in copies[max(n_tiles - slots, 0) :]:
            c.wait()

    specs = [pl.BlockSpec(memory_space=pltpu.VMEM) for _ in lefts + rights]
    args = [*lefts, *rights]
    aliases = {}
    if target is not None:
        aliases = {len(args): 0}
        args.append(target)
        specs.append(pl.BlockSpec(memory_space=pltpu.HBM))
    outs = [shape_of((height, columns), f32)]
    out_specs = [pl.BlockSpec(memory_space=pltpu.HBM)]
    ending_args, scratch = [], []
    if ending is not None:
        ending_args, ending_width = ending
        args += ending_args
        specs += [pl.BlockSpec(memory_space=pltpu.VMEM) for _ in ending_args]
        outs.append(shape_of(ending_args[0].shape, bf16))
        out_specs.append(pl.BlockSpec(memory_space=pltpu.HBM))
        scratch = [pltpu.VMEM(ending_args[0].shape, bf16), pltpu.SemaphoreType.DMA]
    return pl.pallas_call(
        body,
        in_specs=specs,
        out_specs=out_specs,
        out_shape=outs,
        scratch_shapes=[
            pltpu.VMEM((count * tokens, columns), bf16),
            pltpu.VMEM((slots, tile, columns), f32),
            pltpu.SemaphoreType.DMA((slots,)),
            *scratch,
        ],
        input_output_aliases=aliases,
        compiler_params=pltpu.CompilerParams(vmem_limit_bytes=14 * 1024 * 1024),
        cost_estimate=pl.CostEstimate(flops=int(5e8), bytes_accessed=10**6, transcendentals=0),
        name="weight_grad",
    )(*args)


class Plan:
    def __init__(self, n_mp, n_dp):
        ring = ring_of(n_mp, max(n_dp // 2, 1))
        place = {m: i for i, m in enumerate(ring)}
        self.ring = ring
        self.far = far = n_mp // 2
        self.shifts = [0] + [s for d in range(1, far) for s in (-d, d)] + [-far]
        self.event = {s: i for i, s in enumerate(self.shifts)}
        self.per = per = n_mp // n_dp
        block_at = [[ring[(place[m] + s) % n_mp] for s in self.shifts] for m in range(n_mp)]
        event_of = [{b: e for e, b in enumerate(row)} for row in block_at]

        def slots(m, p):
            first = p // 2 * 2 * per
            return sorted(event_of[m][b] for b in range(first, first + 2 * per))

        self.evens = list(range(2, n_dp, 2))
        self.slot_step = [
            max(abs(self.shifts[slots(m, p)[j]]) for m in range(n_mp) for p in range(n_dp))
            for j in range(2 * per)
        ]
        rows = []
        self.column = {}
        for m in range(n_mp):
            for p in range(n_dp):
                row = list(block_at[m])
                for k in self.evens:
                    self.column["send", k] = len(row)
                    row += slots(m, p ^ k)
                mine = [p * per + i for i in range(per)] + [(p ^ 1) * per + i for i in range(per)]
                self.column["own"] = len(row)
                row += [event_of[m][b] for b in mine]
                self.column["sort"] = len(row)
                order = slots(m, p)
                row += [order.index(event_of[m][b]) for b in mine]
                rows.append(row)
        self.table = np.array(rows, np.int32).reshape(n_mp * n_dp, 1, -1)


def on_device(inputs, norm_gain, norm_bias, proj_weight, proj_bias, act_grad):
    height, tokens = inputs.shape
    hidden = proj_weight.shape[1]
    n_mp, n_dp = lax.axis_size("mp"), lax.axis_size("dp")
    width = height * n_mp
    factor = 1.0 / math.sqrt(tokens * n_dp)
    plan = Plan(n_mp, n_dp)
    far, per, shifts, event = plan.far, plan.per, plan.shifts, plan.event
    table = lax.dynamic_index_in_dim(
        jnp.asarray(plan.table), lax.axis_index("mp") * n_dp + lax.axis_index("dp"), 0, keepdims=False
    )
    gain = norm_gain.reshape(n_mp, 1, height)
    bias = norm_bias.reshape(n_mp, 1, height)
    pbias = proj_bias.reshape(1, hidden)
    proj_weight = pltpu.with_memory_space_constraint(proj_weight, pltpu.HBM)

    def swap(value, k):
        return lax.ppermute(value, "dp", [(i, i ^ k) for i in range(n_dp)])

    def along(value, steps):
        pairs = [(plan.ring[i], plan.ring[(i + steps) % n_mp]) for i in range(n_mp)]
        return lax.ppermute(value, "mp", pairs)

    block = {0: inputs}
    for d in range(1, far + 1):
        block[-d] = along(block[-d + 1], 1)
        if d < far:
            block[d] = along(block[d - 1], -1)

    groups = [[0]] + [[event[-d], event[d]] for d in range(1, far)] + [[event[-far]]]
    early = min(2, far - 1)
    groups[: early + 1] = [sum(groups[: early + 1], [])]
    if far == 4:
        window = sums_of([block[0], block[-1], block[1]])
        below = along(window, 3)
        above = along(window, -3)
        sums = [(window, 6), (below, 6), (above, 0), (above, 2)]
    else:
        total, k = sums_of([inputs])[0:2], 1
        while k < n_mp:
            total = total + lax.ppermute(total, "mp", [(i, i ^ k) for i in range(n_mp)])
            k *= 2
        sums = [(total, 0)]

    weights, made = {}, {}

    def keep(events, arrays):
        for e, w in zip(events, arrays):
            weights[e] = pltpu.with_memory_space_constraint(w, pltpu.VMEM)

    first_loads = groups[0][:3]
    keep(first_loads, load_blocks(Loads(table, first_loads, proj_weight, height)))
    more_loads = groups[0][3 : 3 + 2]
    if more_loads:
        keep(more_loads, load_blocks(Loads(table, more_loads, proj_weight, height)))
    acc, sent, slot = None, {k: [] for k in plan.evens}, 0

    def ready_picks(reach):
        nonlocal slot
        more = sum(1 for s in plan.slot_step[slot:] if s <= reach)
        firsts = [plan.column["send", k] + slot for k in plan.evens] if more else []
        slot += more
        return [list(range(first, first + more)) for first in firsts]

    def send(picked):
        for k, value in zip(plan.evens, picked):
            sent[k].append(swap(value, k))

    waiting = []
    for g, events in enumerate(groups[:-1]):
        reach = max(abs(shifts[e]) for e in events)
        picks = ready_picks(reach)
        straight, turned, picked = norm_blocks(
            table, events, [block[shifts[e]] for e in events], gain, bias, sums,
            list(made.items()) if picks else [], picks,
        )
        made.update(zip(events, straight))
        send(picked)
        waiting += zip(events, turned)
        if len(groups) == 3 and g == 0:
            continue
        waiting.sort(key=lambda pair: pair[0] not in weights)
        late = [e for e, _ in waiting if e not in weights]
        loads = Loads(table, late + groups[g + 1], proj_weight, height)
        acc, loaded = preact_add([t for _, t in waiting], [weights[e] for e, _ in waiting if e in weights], acc, loads)
        keep(loads.events, loaded)
        waiting = []

    n_parts = 1
    last = event[-far]
    picks = ready_picks(far)
    pgs, back_sums, stats, made[last], picked = slopes(
        table, last, block[-far], weights[last], gain, bias, sums, acc, pbias, act_grad, n_parts,
        list(made.items()) if picks else [], picks,
    )
    send(picked)

    rights = []
    for pg in pgs:
        pieces = {0: pg}
        for k in plan.evens:
            pieces[k] = swap(pg, k)
        for k in [0, *plan.evens]:
            pieces[k + 1] = swap(pieces[k], 1)
        rights.append([pieces[k] for k in range(n_dp)])
    lefts = {}
    for k in [0, *plan.evens]:
        if k:
            arrived = [(a, j) for a in sent[k] for j in range(a.shape[0] // height)]
            candidates = [(i, a[j * height : (j + 1) * height]) for i, (a, j) in enumerate(arrived)]
            first = plan.column["sort"]
        else:
            candidates = list(made.items())
            first = plan.column["own"]
        mine, other = choose(table, list(range(first, first + 2 * per)), candidates, 2)
        lefts[k] = mine
        lefts[k + 1] = swap(other, 1)
    lefts = [lefts[k] for k in range(n_dp)]

    message = back_blocks([weights[last]], pgs, back_sums, [True])[0]
    up = along(message, 1)
    down = None
    for d in range(far - 1, 0, -1):
        first = down is None
        a, b = back_blocks([weights[event[d]], weights[event[-d]]], pgs, back_sums, [False, first])
        if not first:
            b = add_message(b, down, back_sums)
        down = along(b, -1)
        a = add_message(a, up, back_sums)
        up = along(a, 1)
    own, columns, centred = back_own(table, weights[0], pgs, inputs, gain, stats)
    got = [up] if down is None else [up, down]
    rows = lefts[0].shape[0]
    tiles = 12 if rows % (12 * 16) == 0 else 1
    cuts = [0, 4, tiles] if tiles > 4 > 0 else [0, tiles]
    grad_weight = None
    for span in zip(cuts, cuts[1:]):
        ending = ([own, columns, centred, stats, back_sums, *got], width) if span[1] == tiles else None
        grad_weight, *rest = grad_part(
            lefts, rights[0], grad_weight, span, rows // tiles, factor, ending
        )
    grad_inputs = rest[0]
    return (grad_inputs, grad_weight)


def solution(mesh):
    in_specs = (P("mp", "dp"), P(), P(), P(None, "mp"), P("mp"), P("dp", "mp"))
    out_specs = (P("mp", "dp"), P("dp", "mp"))

    return jax.shard_map(on_device, mesh=mesh, in_specs=in_specs, out_specs=out_specs, check_vma=False)
```
